32 devices in a mesh: dp: 4 (over y, z), ep: 8 (over x, core).
Axes of the slice: x: 4, y: 2, z: 2, core: 2. Of those that a mesh axis runs over, the one named last changes fastest.
The devices are a block of a 4x4x8 slice.
Arguments:
- x_a: bfloat16 [8192, 2048], P(('dp', 'ep')), parts along dimension 0
- route_a: int32 [8192, 6], P(('dp', 'ep')), parts along dimension 0
- gate_a: float32 [8192, 6], P(('dp', 'ep')), parts along dimension 0
- h_b: bfloat16 [8192, 2048], P(('dp', 'ep')), parts along dimension 0
- attn_b: bfloat16 [8192, 2048], P(('dp', 'ep')), parts along dimension 0
- route_b: int32 [8192, 6], P(('dp', 'ep')), parts along dimension 0
- gate_b: float32 [8192, 6], P(('dp', 'ep')), parts along dimension 0
- w_qkv: bfloat16 [2048, 6144], replicated
- w_o: bfloat16 [2048, 2048], replicated
- w_gate: bfloat16 [64, 2048, 1408], P('ep')
- w_up: bfloat16 [64, 2048, 1408], P('ep')
- w_down: bfloat16 [64, 1408, 2048], P('ep')
Outputs:
- output 1: bfloat16 [8192, 2048], P(('dp', 'ep')), parts along dimension 0
- output 2: bfloat16 [8192, 2048], P(('dp', 'ep')), parts along dimension 0
- output 3: bfloat16 [8192, 6144], P(('dp', 'ep')), parts along dimension 0
There are 4 independent parts. The reference program is written for one: setup_inputs(seed, part) draws one part's arguments, and reference() takes and returns one part's arrays. A program takes and returns all parts, laid end to end along the dimension named above; an argument that names none is the same for every part.
All inputs are finite; a program needn't handle non-finite values.
Results may differ from the reference program's by a relative error of at most 0.011069.
Values are sent between devices in bfloat16 or wider.
A program may use at most 768 MiB of HBM per device.

```python
import jax
import jax.numpy as jnp
from jax import lax

MODEL_DIM = 2048
FF_DIM = 1408
NUM_EXPERTS = 64
TOP_K = 6
NUM_HEADS = 16
KV_HEADS = 16
HEAD_DIM = 128
TOKENS_DEV = 256
GROUP_DEVS = 8

CAPACITY = min(TOKENS_DEV, 2 * ((TOKENS_DEV * TOP_K + NUM_EXPERTS - 1) // NUM_EXPERTS))
LOCAL_EXPERTS = NUM_EXPERTS // GROUP_DEVS
QKV_DIM = (NUM_HEADS + 2 * KV_HEADS) * HEAD_DIM
ATTN_DIM = NUM_HEADS * HEAD_DIM
GROUP_ROWS = GROUP_DEVS * TOKENS_DEV
HOT_DEVS = max(1, GROUP_DEVS // 4)


def source_routing(rng_key, dev_order):
    key_local, key_want, key_rows = jax.random.split(rng_key, 3)
    local_order = jax.vmap(lambda sub_key: jax.random.permutation(sub_key, LOCAL_EXPERTS))(jax.random.split(key_local, GROUP_DEVS))
    visits = jnp.arange(NUM_EXPERTS)
    visit_dev = dev_order[visits % GROUP_DEVS]
    visit_expert = visit_dev * LOCAL_EXPERTS + local_order[visit_dev, visits // GROUP_DEVS]
    wanted = jax.random.randint(key_want, (NUM_EXPERTS,), 1, CAPACITY + 1)
    wanted = jnp.where(visits % GROUP_DEVS < HOT_DEVS, CAPACITY, wanted)
    wanted = jnp.where(visits < GROUP_DEVS, 1, wanted)
    wanted = jnp.where(visits == 0, CAPACITY, wanted)
    n_entries = TOKENS_DEV * TOP_K
    first_pass = jnp.clip(n_entries - (jnp.cumsum(wanted) - wanted), 0, wanted)
    room_left = CAPACITY - first_pass
    left_over = n_entries - jnp.sum(first_pass)
    second_pass = jnp.clip(left_over - (jnp.cumsum(room_left) - room_left), 0, room_left)
    run_ends = jnp.cumsum(first_pass + second_pass)
    positions = jnp.arange(n_entries)
    run_index = jnp.sum((run_ends[None, :] <= positions[:, None]).astype(jnp.int32), axis=1)
    choices = visit_expert[run_index].reshape(TOP_K, TOKENS_DEV).T
    return choices[jax.random.permutation(key_rows, TOKENS_DEV)]


def group_routing(rng_key):
    key_order, key_src = jax.random.split(rng_key)
    dev_order = jax.random.permutation(key_order, GROUP_DEVS)
    per_source = jax.vmap(lambda sub_key: source_routing(sub_key, dev_order))(jax.random.split(key_src, GROUP_DEVS))
    return per_source.reshape(GROUP_ROWS, TOP_K).astype(jnp.int32)


def setup_inputs(seed: int = 0, part: int = 0) -> dict:
    root_key = jax.random.key(seed)
    shared_keys = jax.random.split(jax.random.fold_in(root_key, 1), 5)
    part_keys = jax.random.split(jax.random.fold_in(jax.random.fold_in(root_key, 2), part), 7)

    def normal_bf16(sub_key, arr_shape, scale_by):
        return (jax.random.normal(sub_key, arr_shape, jnp.float32) * scale_by).astype(jnp.bfloat16)

    return {
        'x_a': normal_bf16(part_keys[0], (GROUP_ROWS, MODEL_DIM), 1.0),
        'route_a': group_routing(part_keys[1]),
        'gate_a': jax.nn.softmax(jax.random.normal(part_keys[2], (GROUP_ROWS, TOP_K), jnp.float32), axis=-1),
        'h_b': normal_bf16(part_keys[3], (GROUP_ROWS, MODEL_DIM), 1.0),
        'attn_b': normal_bf16(part_keys[4], (GROUP_ROWS, ATTN_DIM), 1.0),
        'route_b': group_routing(part_keys[5]),
        'gate_b': jax.nn.softmax(jax.random.normal(part_keys[6], (GROUP_ROWS, TOP_K), jnp.float32), axis=-1),
        'w_qkv': normal_bf16(shared_keys[0], (MODEL_DIM, QKV_DIM), MODEL_DIM ** -0.5),
        'w_o': normal_bf16(shared_keys[1], (ATTN_DIM, MODEL_DIM), ATTN_DIM ** -0.5),
        'w_gate': normal_bf16(shared_keys[2], (NUM_EXPERTS, MODEL_DIM, FF_DIM), MODEL_DIM ** -0.5),
        'w_up': normal_bf16(shared_keys[3], (NUM_EXPERTS, MODEL_DIM, FF_DIM), MODEL_DIM ** -0.5),
        'w_down': normal_bf16(shared_keys[4], (NUM_EXPERTS, FF_DIM, MODEL_DIM), FF_DIM ** -0.5),
    }


def expert_layer(tokens, route_ids, gate_vals, w_gate, w_up, w_down):
    n_entries = GROUP_ROWS * TOP_K
    per_source = route_ids.reshape(GROUP_DEVS, TOKENS_DEV * TOP_K)
    one_hot = (per_source[:, :, None] == jnp.arange(NUM_EXPERTS)[None, None, :]).astype(jnp.int32)
    slot_rank = jnp.sum((jnp.cumsum(one_hot, axis=1) - 1) * one_hot, axis=2)
    buffer_row = jnp.arange(GROUP_DEVS)[:, None] * CAPACITY + slot_rank
    entry_ids = jnp.arange(n_entries)
    slot_table = jnp.full((NUM_EXPERTS, GROUP_DEVS * CAPACITY), n_entries, jnp.int32)
    slot_table = slot_table.at[per_source.reshape(-1), buffer_row.reshape(-1)].set(entry_ids)
    padded = jnp.concatenate([tokens, jnp.zeros((1, MODEL_DIM), tokens.dtype)], axis=0)

    def one_expert(results, inputs):
        rows_ids, gate_w, up_w, down_w = inputs
        expert_in = padded[rows_ids // TOP_K]
        gate_act = jnp.dot(expert_in, gate_w, preferred_element_type=jnp.float32)
        up_act = jnp.dot(expert_in, up_w, preferred_element_type=jnp.float32)
        hidden = (jax.nn.silu(gate_act) * up_act).astype(jnp.bfloat16)
        expert_out = jnp.dot(hidden, down_w, preferred_element_type=jnp.float32).astype(jnp.bfloat16)
        return results.at[rows_ids].set(expert_out), None

    results = jnp.zeros((n_entries + 1, MODEL_DIM), jnp.bfloat16)
    results = lax.scan(one_expert, results, (slot_table, w_gate, w_up, w_down))[0]
    per_choice = results[:n_entries].reshape(GROUP_ROWS, TOP_K, MODEL_DIM)
    mixture = jnp.zeros((GROUP_ROWS, MODEL_DIM), jnp.float32)
    for choice in range(TOP_K):
        mixture = mixture + gate_vals[:, choice:choice + 1] * per_choice[:, choice].astype(jnp.float32)
    return (tokens.astype(jnp.float32) + mixture).astype(jnp.bfloat16)


def reference(x_a, route_a, gate_a, h_b, attn_b, route_b, gate_b, w_qkv, w_o, w_gate, w_up, w_down):
    out_a = expert_layer(x_a, route_a, gate_a, w_gate, w_up, w_down)
    qkv_b = jnp.dot(h_b, w_qkv, preferred_element_type=jnp.float32).astype(jnp.bfloat16)
    proj_b = jnp.dot(attn_b, w_o, preferred_element_type=jnp.float32).astype(jnp.bfloat16)
    mid_b = (h_b.astype(jnp.float32) + proj_b.astype(jnp.float32)).astype(jnp.bfloat16)
    out_b = expert_layer(mid_b, route_b, gate_b, w_gate, w_up, w_down)
    return (out_a, out_b, qkv_b)
```

```python
import functools

import jax
import jax.numpy as jnp
from jax import lax
from jax.experimental import pallas as pl
from jax.experimental.pallas import tpu as pltpu
from jax.sharding import PartitionSpec as P

F32 = jnp.float32
BF16 = jnp.bfloat16
VMEM_LIMIT = 60 * 1024 * 1024


def routing_tables(route, gate, first_expert, local_n, capacity):
    n_src, _, tok_n = route.shape
    local = route - first_expert
    hits = local[:, :, None, :] == jnp.arange(local_n)[None, None, :, None]
    chosen = jnp.sum(hits.astype(F32), axis=1)
    gates = jnp.sum(jnp.where(hits, gate[:, :, None, :], 0.0), axis=1)
    before = (jnp.arange(tok_n)[:, None] < jnp.arange(tok_n)[None, :]).astype(BF16)
    rank = jnp.dot(chosen.reshape(n_src * local_n, tok_n).astype(BF16), before, preferred_element_type=F32)
    rank = rank.reshape(n_src, local_n, tok_n).astype(jnp.int32)
    rank = jnp.where(chosen > 0, rank, -1)
    slots = jnp.arange(capacity)
    place = (rank[:, :, None, :] == slots[None, None, :, None]).astype(BF16)
    place = place.reshape(n_src, local_n * capacity, tok_n)
    hi = lax.reduce_precision(gates, 8, 7)
    rest = gates - hi
    mid = lax.reduce_precision(rest, 8, 7)
    low = rest - mid
    parts = jnp.stack([hi, mid, low], axis=1)
    parts = jnp.swapaxes(parts, 2, 3)
    rank_t = jnp.swapaxes(rank, 1, 2)
    combine = jnp.where(
        rank_t[:, None, :, :, None] == slots[None, None, None, None, :], parts[:, :, :, :, None], 0.0
    ).astype(BF16)
    return place, combine.reshape(n_src, 3 * tok_n, local_n * capacity)


def dispatch(place, tokens, local_n, capacity):
    n_src, n_slots, tok_n = place.shape
    dim = tokens.shape[1]

    def body(place_ref, tok_ref, out_ref):
        rows = jnp.dot(place_ref[0], tok_ref[...], preferred_element_type=F32).astype(BF16)
        out_ref[:, 0] = rows.reshape(local_n, capacity, dim)

    return pl.pallas_call(
        body,
        grid=(n_src,),
        in_specs=[
            pl.BlockSpec((1, n_slots, tok_n), lambda s: (s, 0, 0)),
            pl.BlockSpec((tok_n, dim), lambda s: (s, 0)),
        ],
        out_specs=pl.BlockSpec((local_n, 1, capacity, dim), lambda s: (0, s, 0, 0)),
        out_shape=jax.ShapeDtypeStruct((local_n, n_src, capacity, dim), BF16),
        compiler_params=pltpu.CompilerParams(vmem_limit_bytes=VMEM_LIMIT),
        cost_estimate=pl.CostEstimate(
            flops=2 * n_src * n_slots * tok_n * dim, bytes_accessed=22_000_000, transcendentals=0
        ),
        name="dispatch",
    )(place, tokens)


def gate_up(rows, w_gate, w_up):
    local_n, row_n, dim = rows.shape
    ff = w_gate.shape[2]
    wide = 256
    n_full = ff // wide

    def body(rows_ref, wg_ref, wu_ref, out_ref):
        x = rows_ref[0]
        for i in range(n_full):
            cols = slice(i * wide, (i + 1) * wide)
            g = jnp.dot(x, wg_ref[0, :, cols], preferred_element_type=F32)
            u = jnp.dot(x, wu_ref[0, :, cols], preferred_element_type=F32)
            out_ref[0, :, cols] = (jax.nn.silu(g) * u).astype(BF16)
        if n_full * wide < ff:
            tail = ff - n_full * wide
            both = jnp.concatenate([wg_ref[0, :, n_full * wide :], wu_ref[0, :, n_full * wide :]], axis=1)
            gu = jnp.dot(x, both, preferred_element_type=F32)
            out_ref[0, :, n_full * wide :] = (jax.nn.silu(gu[:, :tail]) * gu[:, tail:]).astype(BF16)

    return pl.pallas_call(
        body,
        grid=(local_n,),
        in_specs=[
            pl.BlockSpec((1, row_n, dim), lambda e: (e, 0, 0)),
            pl.BlockSpec((1, dim, ff), lambda e: (e, 0, 0)),
            pl.BlockSpec((1, dim, ff), lambda e: (e, 0, 0)),
        ],
        out_specs=pl.BlockSpec((1, row_n, ff), lambda e: (e, 0, 0)),
        out_shape=jax.ShapeDtypeStruct((local_n, row_n, ff), BF16),
        compiler_params=pltpu.CompilerParams(vmem_limit_bytes=VMEM_LIMIT),
        cost_estimate=pl.CostEstimate(
            flops=4 * local_n * row_n * dim * ff,
            bytes_accessed=2 * local_n * (2 * dim * ff + row_n * (dim + ff)),
            transcendentals=local_n * row_n * ff,
        ),
        name="gate_up",
    )(rows, w_gate, w_up)


def down_mix(hidden, w_down, combine, chunk, n_chunks, capacity):
    local_n, row_n, ff = hidden.shape
    dim = w_down.shape[2]
    n_src, tok3, n_slots = combine.shape
    tok_n = tok3 // 3
    cols = dim // n_chunks

    def body(hid_ref, wd_ref, comb_ref, out_ref, y_ref):
        e = pl.program_id(0)
        y = jnp.dot(hid_ref[0], wd_ref[0], preferred_element_type=F32).astype(BF16)
        y_ref[:, e] = y.reshape(n_src, capacity, cols)

        @pl.when(e == local_n - 1)
        def _():
            for s in range(n_src):
                ys = y_ref[s].reshape(n_slots, cols)
                mix = jnp.dot(comb_ref[s], ys, preferred_element_type=F32)
                out_ref[s * tok_n : (s + 1) * tok_n] = (
                    mix[:tok_n] + mix[tok_n : 2 * tok_n] + mix[2 * tok_n :]
                )

    return pl.pallas_call(
        body,
        grid=(local_n,),
        in_specs=[
            pl.BlockSpec((1, row_n, ff), lambda e: (e, 0, 0)),
            pl.BlockSpec((1, ff, cols), lambda e: (e, 0, chunk)),
            pl.BlockSpec((n_src, tok3, n_slots), lambda e: (0, 0, 0)),
        ],
        out_specs=pl.BlockSpec((n_src * tok_n, cols), lambda e: (0, 0)),
        out_shape=jax.ShapeDtypeStruct((n_src * tok_n, cols), F32),
        scratch_shapes=[pltpu.VMEM((n_src, local_n, capacity, cols), BF16)],
        compiler_params=pltpu.CompilerParams(vmem_limit_bytes=VMEM_LIMIT),
        cost_estimate=pl.CostEstimate(
            flops=2 * local_n * row_n * ff * cols + 2 * n_src * tok3 * n_slots * cols,
            bytes_accessed=2 * local_n * (ff * cols + row_n * ff) + 4 * n_src * tok_n * cols,
            transcendentals=0,
        ),
        name="down_mix",
    )(hidden, w_down, combine)


def solution(mesh):
    n_devs = mesh.shape['ep']

    def local_step(x_a, route_a, gate_a, h_b, attn_b, route_b, gate_b, w_qkv, w_o, w_gate, w_up, w_down):
        tok_n, dim = x_a.shape
        top_k = route_a.shape[1]
        local_n = w_gate.shape[0]
        n_experts = local_n * n_devs
        capacity = min(tok_n, 2 * ((tok_n * top_k + n_experts - 1) // n_experts))
        me = lax.axis_index('ep')

        all_a = lax.all_gather(x_a, 'ep', axis=0, tiled=True)
        proj_b = jnp.dot(attn_b, w_o, preferred_element_type=F32).astype(BF16)
        mid_b = (h_b.astype(F32) + proj_b.astype(F32)).astype(BF16)
        all_b = lax.all_gather(mid_b, 'ep', axis=0, tiled=True)

        meta = jnp.concatenate([route_a.astype(F32).T, gate_a.T, route_b.astype(F32).T, gate_b.T], axis=0)
        meta = lax.all_gather(meta, 'ep', axis=0)
        k = top_k
        tables_a = routing_tables(meta[:, :k].astype(jnp.int32), meta[:, k : 2 * k], me * local_n, local_n, capacity)
        tables_b = routing_tables(
            meta[:, 2 * k : 3 * k].astype(jnp.int32), meta[:, 3 * k :], me * local_n, local_n, capacity
        )
        qkv_b = jnp.dot(h_b, w_qkv, preferred_element_type=F32).astype(BF16)

        def moe(tokens, all_tokens, tables):
            place, combine = tables
            n_chunks = 4
            rows = dispatch(place, all_tokens, local_n, capacity)
            hidden = gate_up(rows.reshape(local_n, n_devs * capacity, dim), w_gate, w_up)
            parts = []
            for chunk in range(n_chunks):
                part = down_mix(hidden, w_down, combine, chunk, n_chunks, capacity)
                parts.append(lax.psum_scatter(part, 'ep', scatter_dimension=0, tiled=True))
            mixture = jnp.concatenate(parts, axis=1)
            return (tokens.astype(F32) + mixture).astype(BF16)

        return moe(x_a, all_a, tables_a), moe(mid_b, all_b, tables_b), qkv_b

    row_spec = P(('dp', 'ep'), None)
    full_spec = P(None, None)
    expert_spec = P('ep', None, None)
    return jax.shard_map(
        local_step,
        mesh=mesh,
        in_specs=(row_spec, row_spec, row_spec, row_spec, row_spec, row_spec, row_spec, full_spec, full_spec, expert_spec, expert_spec, expert_spec),
        out_specs=(row_spec, row_spec, row_spec),
        check_vma=False,
    )
```

```python
import jax
import jax.numpy as jnp
from jax import lax
from jax.experimental import pallas as pl
from jax.experimental.pallas import tpu as pltpu
from jax.sharding import PartitionSpec as P

F32 = jnp.float32
BF16 = jnp.bfloat16
VMEM_LIMIT = 67_000_000
WIDE = 256
SLOTS = 4
CHUNKS = 4


def rem(a, b):
    return lax.rem(a, jnp.int32(b))


def div(a, b):
    return lax.div(a, jnp.int32(b))


def moe_kernel(
    capacity,
    x_a, h_b, attn_b, meta, w_qkv, w_o, w_gate, w_up, w_down,
    out_a, out_b, qkv, land,
    wbuf, rows, hidden, src_rows, expert_out, mixer, partial, pair, transit, near, out_stage, own_stage, table,
    w_sem, gather_send, gather_recv, meta_send, meta_recv, load_sem, stage_sem, own_sem,
    pair_send, pair_recv, far_send, far_recv, near_send, near_recv, credit,
):
    n_devs = land.shape[1]
    n_chips = n_devs // 2
    tok_n, dim = x_a.shape
    half_n = tok_n // 2
    local_n, row_n, ff = hidden.shape
    n_slots = local_n * capacity
    cols = dim // CHUNKS
    half = cols // 2
    n_full, tail = ff // WIDE, ff % WIDE
    gu_tiles = n_full + 1

    me = lax.axis_index('ep')
    chip, core = div(me, 2), rem(me, 2)
    partner = me + 1 - 2 * core
    right, left = rem(me + 2, n_devs), rem(me + n_devs - 2, n_devs)
    sides = (right, left)
    chip_right, chip_left, chip_far = rem(chip + 1, n_chips), rem(chip + n_chips - 1, n_chips), rem(chip + 2, n_chips)
    chip_side = (chip_right, chip_left)
    far = 2 * chip_far + core

    def remote(src, dst, send, recv, dev):
        return pltpu.make_async_remote_copy(
            src_ref=src, dst_ref=dst, send_sem=send, recv_sem=recv, device_id={'ep': dev},
            device_id_type=pl.DeviceIdType.MESH,
        )

    def sl(start, size):
        return pl.ds(pl.multiple_of(start, size), size)

    def tile_copies(phase, i):
        slot = rem(i, SLOTS)
        if phase in ('proj', 'qkv'):
            w = w_o if phase == 'proj' else w_qkv
            return ((None, [(w.at[:, sl(i * cols, cols)], wbuf.at[slot, :, 0:cols], w_sem.at[slot, 0])]),)
        if phase == 'down':
            n, e = div(i, local_n), rem(i, local_n)
            return ((None, [(w_down.at[e, :, sl(n * cols, cols)], wbuf.at[slot, 0:ff, 0:cols], w_sem.at[slot, 0])]),)
        e, t = div(i, gu_tiles), rem(i, gu_tiles)
        full = [
            (w_gate.at[e, :, sl(t * WIDE, WIDE)], wbuf.at[slot, :, 0:WIDE], w_sem.at[slot, 0]),
            (w_up.at[e, :, sl(t * WIDE, WIDE)], wbuf.at[slot, :, WIDE : 2 * WIDE], w_sem.at[slot, 1]),
        ]
        part = [
            (w_gate.at[e, :, n_full * WIDE : ff], wbuf.at[slot, :, 0:tail], w_sem.at[slot, 0]),
            (w_up.at[e, :, n_full * WIDE : ff], wbuf.at[slot, :, tail : 2 * tail], w_sem.at[slot, 1]),
        ]
        return ((t < n_full, full), (t == n_full, part))

    def fetch(phase, i):
        for cond, copies in tile_copies(phase, i):
            def go(copies=copies):
                for c in copies:
                    pltpu.make_async_copy(*c).start()
            if cond is None:
                go()
            else:
                pl.when(cond)(go)

    def arrive(phase, i, which=0):
        for c in tile_copies(phase, i)[which][1]:
            pltpu.make_async_copy(*c).wait()

    count = {'proj': CHUNKS, 'qkv': qkv.shape[1] // cols, 'gate_up': local_n * gu_tiles, 'down': CHUNKS * local_n}
    ahead = SLOTS - 1

    def next_tile(phase, following, i):
        @pl.when(i + ahead < count[phase])
        def _():
            fetch(phase, i + ahead)

        if following is not None:
            @pl.when(i + ahead >= count[phase])
            def _():
                fetch(following, i + ahead - count[phase])

    def own(m):
        return x_a if m == 0 else land.at[m, me]

    def rows_half(ref, hf):
        return ref.at[hf * half_n : (hf + 1) * half_n]

    def g_partner(m):
        return remote(own(m), land.at[m, me], gather_send.at[m, 0], gather_recv.at[m, 0], partner)

    def g_near(m, d, hf):
        k = 1 + 2 * d + hf
        return remote(
            rows_half(own(m), hf), rows_half(land.at[m, me], hf), gather_send.at[m, k], gather_recv.at[m, k], sides[d]
        )

    def g_forward(m, d):
        block = rows_half(land.at[m, sides[1 - d]], d)
        return remote(block, block, gather_send.at[m, 5 + d], gather_recv.at[m, 5 + d], sides[d])

    def g_pass(m, d):
        block = land.at[m, sides[1 - d]]
        return remote(block, block, gather_send.at[m, 7 + d], gather_recv.at[m, 7 + d], partner)

    def g_pass_far(m, d):
        block = rows_half(land.at[m, far], d)
        return remote(block, block, gather_send.at[m, 9 + d], gather_recv.at[m, 9 + d], partner)

    def gather_start(m):
        g_partner(m).start()
        for step in range(2):
            for d in range(2):
                g_near(m, d, d if step == 0 else 1 - d).start()

    def gather_forward(m):
        for d in range(2):
            g_near(m, d, d).wait_recv()
            g_forward(m, d).start()

    def gather_pass(m):
        for d in range(2):
            g_near(m, d, 1 - d).wait_recv()
            g_pass(m, d).start()

    def gather_near_done(m):
        g_partner(m).wait_recv()
        for d in range(2):
            g_pass(m, d).wait_recv()

    def gather_pass_far(m):
        for d in range(2):
            g_forward(m, d).wait_recv()
            g_pass_far(m, d).start()

    def gather_done(m):
        for d in range(2):
            g_pass_far(m, d).wait_recv()
        g_partner(m).wait_send()
        for d in range(2):
            g_near(m, d, 0).wait_send()
            g_near(m, d, 1).wait_send()
            g_forward(m, d).wait_send()
            g_pass(m, d).wait_send()
            g_pass_far(m, d).wait_send()

    def source_at(k):
        kk = div(k, 2)
        off = kk + div(kk, 2) - 2 * div(kk, 3)
        return 2 * rem(chip + off, n_chips) + rem(k, 2)

    def load(m, k):
        return pltpu.make_async_copy(land.at[m, source_at(k)], src_rows.at[rem(k, 2)], load_sem.at[rem(k, 2)])

    def dispatch(m, lo, hi):
        load(m, jnp.int32(lo)).start()

        def body(k, carry):
            @pl.when(k + 1 < hi)
            def _():
                load(m, k + 1).start()

            s, slot = source_at(k), rem(k, 2)
            load(m, k).wait()
            rank = table[s, m, 0:local_n]
            slots = lax.broadcasted_iota(jnp.int32, (capacity, tok_n), 0).astype(F32)
            pick = jnp.concatenate(
                [jnp.where(rank[e : e + 1] == slots, 1.0, 0.0).astype(BF16) for e in range(local_n)], axis=0
            )
            for j in range(CHUNKS):
                part = slice(j * cols, (j + 1) * cols)
                got = jnp.dot(pick, src_rows[slot, :, part], preferred_element_type=F32).astype(BF16)
                for e in range(local_n):
                    rows[e, pl.ds(pl.multiple_of(s * capacity, capacity), capacity), part] = got[
                        e * capacity : (e + 1) * capacity
                    ]
            return carry

        lax.fori_loop(jnp.int32(lo), jnp.int32(hi), body, 0)

    def make_mixer(m):
        lane = lax.broadcasted_iota(jnp.int32, (2 * local_n, n_slots), 1)
        line = lax.broadcasted_iota(jnp.int32, (2 * local_n, n_slots), 0)

        def spread(first):
            low = (line - first) * capacity
            inside = (line >= first) & (line < first + local_n) & (lane >= low) & (lane < low + capacity)
            return jnp.where(inside, 1.0, 0.0).astype(BF16)

        spread_rank, spread_gate = spread(0), spread(local_n)
        at = lax.broadcasted_iota(jnp.int32, (tok_n, n_slots), 1)
        base = jnp.zeros_like(at)
        for e in range(1, local_n):
            base = base + jnp.where(at >= e * capacity, capacity, 0)
        at = (at - base).astype(F32)

        def body(s, carry):
            value = table[s, m]
            hi = value.astype(BF16)
            rest = value - hi.astype(F32)
            mid = rest.astype(BF16)
            low = (rest - mid.astype(F32)).astype(BF16)

            def turn(v, e):
                return lax.dot_general(v, e, (((0,), (0,)), ((), ())), preferred_element_type=F32)

            here = turn(hi, spread_rank) == at
            for k, v in enumerate((hi, mid, low)):
                mixer[s, k * tok_n : (k + 1) * tok_n] = jnp.where(here, turn(v, spread_gate), 0.0).astype(BF16)
            return carry

        lax.fori_loop(jnp.int32(0), jnp.int32(n_devs), body, 0)

    def r_pair(n):
        return remote(partial.at[1 - core], pair.at[n], pair_send.at[n], pair_recv.at[n], partner)

    def r_far(n, d):
        return remote(pair.at[n, chip_far, d], transit.at[n, d], far_send.at[n, d], far_recv.at[n, d], sides[d])

    def r_near(n, d, hf):
        return remote(
            pair.at[n, chip_side[d], hf], near.at[n, d, hf], near_send.at[n, d, hf], near_recv.at[n, d, hf], sides[d]
        )

    def own_rows(m, n):
        return pltpu.make_async_copy(
            land.at[m, me, :, sl(n * cols, cols)], own_stage.at[n], own_sem.at[n]
        )

    def out_copy(m, n):
        return pltpu.make_async_copy(
            out_stage.at[n], (out_a, out_b)[m].at[:, sl(n * cols, cols)], stage_sem.at[n]
        )

    def back_pair(n):
        r_pair(n).start()

    def back_far(n):
        r_pair(n).wait()

        def body(k, carry):
            for hf in range(2):
                pair[n, k, hf] += partial[core, k, hf]
            return carry

        lax.fori_loop(jnp.int32(0), jnp.int32(n_chips), body, 0)
        for d in range(2):
            r_far(n, d).start()
        for d in range(2):
            r_near(n, d, 1 - d).start()

    def back_near(m, n):
        for d in range(2):
            r_far(n, d).wait_recv()
            pair[n, chip_side[d], d] += transit[n, d]
            r_near(n, d, d).start()
        own_rows(m, n).start()

    def back_out(m, n):
        for d in range(2):
            r_far(n, d).wait_send()
            for hf in range(2):
                r_near(n, d, hf).wait()
        own_rows(m, n).wait()
        if m == 1:
            out_copy(0, n).wait()
        for hf in range(2):
            part = slice(hf * half, (hf + 1) * half)
            total = pair[n, chip, hf] + near[n, 0, hf] + near[n, 1, hf]
            out_stage[n, :, part] = (own_stage[n, :, part].astype(F32) + total).astype(BF16)
        out_copy(m, n).start()

    for k in range(3):
        fetch('proj', jnp.int32(k))
    barrier = pltpu.get_barrier_semaphore()
    for k in range(1, n_devs):
        pl.semaphore_signal(
            barrier, inc=1, device_id={'ep': rem(me + k, n_devs)}, device_id_type=pl.DeviceIdType.MESH
        )
    attn_in = pltpu.make_async_copy(attn_b, rows.at[0, 0:tok_n], load_sem.at[0])
    h_in = pltpu.make_async_copy(h_b, rows.at[1, 0:tok_n], load_sem.at[1])
    x_in = pltpu.make_async_copy(x_a, rows.at[3, 0:tok_n], own_sem.at[0])
    attn_in.start()
    h_in.start()
    x_in.start()
    pl.semaphore_wait(barrier, n_devs - 1)

    def m_send(k):
        to = rem(me + k, n_devs)
        return remote(meta.at[to], table.at[me], meta_send.at[k], meta_recv.at[k], to)

    for k in range(1, n_devs):
        m_send(k).start()
    gather_start(0)
    table[me] = meta[me]
    x_in.wait()
    x_put = pltpu.make_async_copy(rows.at[3, 0:tok_n], land.at[0, me], own_sem.at[0])
    x_put.start()
    attn_in.wait()
    h_in.wait()

    def proj_tile(j, carry):
        arrive('proj', j)
        next_tile('proj', 'qkv', j)
        part = sl(j * cols, cols)
        got = jnp.dot(rows[0, 0:tok_n], wbuf[rem(j, SLOTS), :, 0:cols], preferred_element_type=F32).astype(BF16)
        rows[2, 0:tok_n, part] = (rows[1, 0:tok_n, part].astype(F32) + got.astype(F32)).astype(BF16)
        return carry

    lax.fori_loop(jnp.int32(0), jnp.int32(count['proj']), proj_tile, 0)
    mid_put = pltpu.make_async_copy(rows.at[2, 0:tok_n], land.at[1, me], own_sem.at[1])
    mid_put.start()

    def qkv_copy(j):
        return pltpu.make_async_copy(
            out_stage.at[rem(j, CHUNKS)], qkv.at[:, sl(j * cols, cols)], stage_sem.at[rem(j, CHUNKS)]
        )

    def qkv_tile(j, carry):
        arrive('qkv', j)
        next_tile('qkv', 'gate_up', j)

        @pl.when(j >= CHUNKS)
        def _():
            qkv_copy(j - CHUNKS).wait()

        got = jnp.dot(rows[1, 0:tok_n], wbuf[rem(j, SLOTS), :, 0:cols], preferred_element_type=F32)
        out_stage[rem(j, CHUNKS)] = got.astype(BF16)
        qkv_copy(j).start()

        @pl.when(j == count['qkv'] // 2)
        def _():
            gather_forward(0)

        return carry

    lax.fori_loop(jnp.int32(0), jnp.int32(count['qkv']), qkv_tile, 0)
    x_put.wait()
    mid_put.wait()
    for j in range(count['qkv'] - CHUNKS, count['qkv']):
        qkv_copy(jnp.int32(j)).wait()
    for k in range(1, n_devs):
        m_send(k).wait()
    make_mixer(0)
    gather_pass(0)
    gather_start(1)
    gather_near_done(0)

    for m in range(2):
        dispatch(m, 0, n_devs - 2)
        if m == 0:
            gather_pass_far(0)
            gather_done(0)
        dispatch(m, n_devs - 2, n_devs)
        if m == 1:
            make_mixer(1)
            back_far(jnp.int32(CHUNKS - 1))
            back_near(0, jnp.int32(1))

        def gu_expert(e, carry, m=m):
            def full_tile(t, carry):
                i = e * gu_tiles + t
                arrive('gate_up', i, 0)
                next_tile('gate_up', 'down', i)
                slot = rem(i, SLOTS)
                g = jnp.dot(rows[e], wbuf[slot, :, 0:WIDE], preferred_element_type=F32)
                u = jnp.dot(rows[e], wbuf[slot, :, WIDE : 2 * WIDE], preferred_element_type=F32)
                hidden[e, :, sl(t * WIDE, WIDE)] = (jax.nn.silu(g) * u).astype(BF16)
                return carry

            lax.fori_loop(jnp.int32(0), jnp.int32(n_full), full_tile, 0)
            i = e * gu_tiles + n_full
            arrive('gate_up', i, 1)
            next_tile('gate_up', 'down', i)
            gu = jnp.dot(rows[e], wbuf[rem(i, SLOTS), :, 0 : 2 * tail], preferred_element_type=F32)
            hidden[e, :, n_full * WIDE : ff] = (jax.nn.silu(gu[:, 0:tail]) * gu[:, tail : 2 * tail]).astype(BF16)

            if m == 0:
                events = {2: [lambda: gather_forward(1)], 4: [lambda: gather_pass(1)]}
            else:
                events = {
                    1: [lambda: back_near(0, jnp.int32(2))],
                    3: [lambda: back_out(0, jnp.int32(0))],
                    4: [lambda: back_near(0, jnp.int32(3))],
                    5: [lambda: back_out(0, jnp.int32(1))],
                    6: [lambda: back_out(0, jnp.int32(2))],
                    7: [lambda: back_out(0, jnp.int32(3))],
                }
            for at, steps in events.items():
                def run(steps=steps):
                    for step in steps:
                        step()
                pl.when(e == at)(run)
            return carry

        lax.fori_loop(jnp.int32(0), jnp.int32(local_n), gu_expert, 0)
        if m == 0:
            gather_pass_far(1)
        else:
            for dev in (partner, right, left):
                pl.semaphore_signal(credit, inc=1, device_id={'ep': dev}, device_id_type=pl.DeviceIdType.MESH)

        def down_chunk(n, carry, m=m):
            def tile(e, carry):
                i = n * local_n + e
                arrive('down', i)
                next_tile('down', 'gate_up' if m == 0 else None, i)
                y = jnp.dot(hidden[e], wbuf[rem(i, SLOTS), 0:ff, 0:cols], preferred_element_type=F32).astype(BF16)
                expert_out[:, pl.ds(pl.multiple_of(e * capacity, capacity), capacity), :] = y.reshape(
                    n_devs, capacity, cols
                )

                @pl.when((e == 2) & (n == 2))
                def _():
                    back_near(m, jnp.int32(0))

                @pl.when((e == 5) & (n >= 1))
                def _():
                    back_far(n - 1)

                return carry

            lax.fori_loop(jnp.int32(0), jnp.int32(local_n), tile, 0)

            def mix(s, carry):
                for hf in range(2):
                    ys = expert_out[s, :, hf * half : (hf + 1) * half]
                    got = jnp.dot(mixer[s], ys, preferred_element_type=F32)
                    partial[rem(s, 2), div(s, 2), hf] = (
                        got[0:tok_n] + got[tok_n : 2 * tok_n] + got[2 * tok_n : 3 * tok_n]
                    )
                return carry

            lax.fori_loop(jnp.int32(0), jnp.int32(n_devs), mix, 0)
            if m == 1:
                @pl.when(n == 0)
                def _():
                    pl.semaphore_wait(credit, 3)

            back_pair(n)
            return carry

        lax.fori_loop(jnp.int32(0), jnp.int32(CHUNKS), down_chunk, 0)
        if m == 0:
            gather_near_done(1)
            gather_done(1)

    back_near(1, jnp.int32(1))
    back_far(jnp.int32(CHUNKS - 1))
    back_near(1, jnp.int32(2))
    back_out(1, jnp.int32(0))
    back_near(1, jnp.int32(3))
    for n in range(1, CHUNKS):
        back_out(1, jnp.int32(n))
    for n in range(CHUNKS):
        out_copy(1, jnp.int32(n)).wait()


def own_table(route, gate, n_experts):
    tok_n = route.shape[0]
    hits = route.T[:, None, :] == jnp.arange(n_experts)[None, :, None]
    chosen = jnp.any(hits, axis=0)
    gates = jnp.sum(jnp.where(hits, gate.T[:, None, :], 0.0), axis=0)
    before = (jnp.arange(tok_n)[:, None] < jnp.arange(tok_n)[None, :]).astype(BF16)
    rank = jnp.dot(chosen.astype(BF16), before, preferred_element_type=F32)
    return jnp.where(chosen, rank, -1.0), gates


def solution(mesh):
    n_devs = mesh.shape['ep']

    def local_step(x_a, route_a, gate_a, h_b, attn_b, route_b, gate_b, w_qkv, w_o, w_gate, w_up, w_down):
        tok_n, dim = x_a.shape
        top_k = route_a.shape[1]
        local_n, _, ff = w_gate.shape
        n_experts = local_n * n_devs
        capacity = min(tok_n, 2 * ((tok_n * top_k + n_experts - 1) // n_experts))
        row_n, n_slots, cols = n_devs * capacity, local_n * capacity, dim // CHUNKS
        half, n_chips = cols // 2, n_devs // 2

        halves = []
        for route, gate in ((route_a, gate_a), (route_b, gate_b)):
            rank, gates = own_table(route, gate, n_experts)
            halves.append(
                jnp.concatenate(
                    [rank.reshape(n_devs, local_n, tok_n), gates.reshape(n_devs, local_n, tok_n)], axis=1
                )
            )
        meta = jnp.stack(halves, axis=1)

        any_spec = pl.BlockSpec(memory_space=pl.ANY)
        dma = pltpu.SemaphoreType.DMA

        def body(*refs):
            moe_kernel(capacity, *refs)

        flops = 2 * (6 * local_n * row_n * dim * ff + 8 * n_devs * n_slots * tok_n * dim) + 2 * tok_n * dim * 4 * dim
        out_a, out_b, qkv_b, _ = pl.pallas_call(
            body,
            in_specs=[any_spec, any_spec, any_spec, pl.BlockSpec(memory_space=pltpu.VMEM)] + [any_spec] * 5,
            out_specs=[any_spec] * 4,
            out_shape=[
                jax.ShapeDtypeStruct((tok_n, dim), BF16),
                jax.ShapeDtypeStruct((tok_n, dim), BF16),
                jax.ShapeDtypeStruct((tok_n, w_qkv.shape[1]), BF16),
                jax.ShapeDtypeStruct((2, n_devs, tok_n, dim), BF16),
            ],
            scratch_shapes=[
                pltpu.VMEM((SLOTS, dim, max(cols, 2 * WIDE)), BF16),
                pltpu.VMEM((local_n, row_n, dim), BF16),
                pltpu.VMEM((local_n, row_n, ff), BF16),
                pltpu.VMEM((2, tok_n, dim), BF16),
                pltpu.VMEM((n_devs, n_slots, cols), BF16),
                pltpu.VMEM((n_devs, 3 * tok_n, n_slots), BF16),
                pltpu.VMEM((2, n_chips, 2, tok_n, half), F32),
                pltpu.VMEM((CHUNKS, n_chips, 2, tok_n, half), F32),
                pltpu.VMEM((CHUNKS, 2, tok_n, half), F32),
                pltpu.VMEM((CHUNKS, 2, 2, tok_n, half), F32),
                pltpu.VMEM((CHUNKS, tok_n, cols), BF16),
                pltpu.VMEM((CHUNKS, tok_n, cols), BF16),
                pltpu.VMEM((n_devs, 2, 2 * local_n, tok_n), F32),
                dma((SLOTS, 2)),
                dma((2, 11)),
                dma((2, 11)),
                dma((n_devs,)),
                dma((n_devs,)),
                dma((2,)),
                dma((CHUNKS,)),
                dma((CHUNKS,)),
                dma((CHUNKS,)),
                dma((CHUNKS,)),
                dma((CHUNKS, 2)),
                dma((CHUNKS, 2)),
                dma((CHUNKS, 2, 2)),
                dma((CHUNKS, 2, 2)),
                pltpu.SemaphoreType.REGULAR,
            ],
            compiler_params=pltpu.CompilerParams(
                collective_id=0, has_side_effects=True, vmem_limit_bytes=VMEM_LIMIT
            ),
            cost_estimate=pl.CostEstimate(flops=flops, bytes_accessed=400_000_000, transcendentals=0),
            name="moe_step",
        )(x_a, h_b, attn_b, meta, w_qkv, w_o, w_gate, w_up, w_down)
        return out_a, out_b, qkv_b

    row_spec = P(('dp', 'ep'), None)
    full_spec = P(None, None)
    expert_spec = P('ep', None, None)
    return jax.shard_map(
        local_step,
        mesh=mesh,
        in_specs=(row_spec, row_spec, row_spec, row_spec, row_spec, row_spec, row_spec, full_spec, full_spec, expert_spec, expert_spec, expert_spec),
        out_specs=(row_spec, row_spec, row_spec),
        check_vma=False,
    )
```

```python
import jax
import jax.numpy as jnp
from jax import lax
from jax.experimental import pallas as pl
from jax.experimental.pallas import tpu as pltpu
from jax.sharding import PartitionSpec as P

F32 = jnp.float32
BF16 = jnp.bfloat16
VMEM_LIMIT = 67_000_000
WIDE = 256
SLOTS = 3
CHUNKS = 4


def rem(a, b):
    return lax.rem(a, jnp.int32(b))


def div(a, b):
    return lax.div(a, jnp.int32(b))


def moe_kernel(
    capacity,
    x_a, h_b, attn_b, route_a, gate_a, route_b, gate_b, w_qkv, w_o, w_gate, w_up, w_down,
    out_a, out_b, qkv, land,
    wbuf, rows, hidden, meta, expert_out, mixer, partial, pair, transit, near, out_stage, own_stage, table,
    w_sem, gather_send, gather_recv, meta_send, meta_recv, load_sem, stage_sem, own_sem,
    pair_send, pair_recv, far_send, far_recv, near_send, near_recv, credit,
):
    n_devs = land.shape[1]
    n_chips = n_devs // 2
    tok_n, dim = x_a.shape
    half_n = tok_n // 2
    local_n, row_n, ff = hidden.shape
    n_slots = local_n * capacity
    cols = dim // CHUNKS
    half = cols // 2
    n_full, tail = ff // WIDE, ff % WIDE
    gu_tiles = n_full + 1

    me = lax.axis_index('ep')
    chip, core = div(me, 2), rem(me, 2)
    partner = me + 1 - 2 * core
    right, left = rem(me + 2, n_devs), rem(me + n_devs - 2, n_devs)
    sides = (right, left)
    chip_right, chip_left, chip_far = rem(chip + 1, n_chips), rem(chip + n_chips - 1, n_chips), rem(chip + 2, n_chips)
    chip_side = (chip_right, chip_left)
    far = 2 * chip_far + core

    def remote(src, dst, send, recv, dev):
        return pltpu.make_async_remote_copy(
            src_ref=src, dst_ref=dst, send_sem=send, recv_sem=recv, device_id={'ep': dev},
            device_id_type=pl.DeviceIdType.MESH,
        )

    def sl(start, size):
        return pl.ds(pl.multiple_of(start, size), size)

    pairs_of = {'proj': CHUNKS // 2, 'qkv': qkv.shape[1] // cols // 2, 'down': CHUNKS * local_n // 2}
    gu_pairs = gu_tiles // 2
    pairs_of['gate_up'] = local_n * gu_pairs
    stream, total = [], 0
    for kind in ('proj', 'qkv', 'gate_up', 'down', 'gate_up', 'down'):
        stream.append((kind, total, pairs_of[kind]))
        total += pairs_of[kind]

    def slot_of(ph, q):
        return rem(q + stream[ph][1], SLOTS)

    def tile_copies(ph, q, r=0):
        kind = stream[ph][0]
        slot = slot_of(ph, q * gu_pairs + r if kind == 'gate_up' else q)
        out = []
        for k in range(2):
            buf, sem = wbuf.at[slot, k], w_sem.at[slot, k]
            if kind in ('proj', 'qkv'):
                w = w_o if kind == 'proj' else w_qkv
                out.append((w.at[:, sl((2 * q + k) * cols, cols)], buf.at[:, 0:cols], sem.at[0]))
            elif kind == 'down':
                n, e = div(q, local_n // 2), rem(q, local_n // 2) * 2 + k
                out.append((w_down.at[e, :, sl(n * cols, cols)], buf.at[0:ff, 0:cols], sem.at[0]))
            else:
                t = 2 * r + k
                lo, size = t * WIDE, WIDE if t < n_full else tail
                out.append((w_gate.at[q, :, lo : lo + size], buf.at[:, 0:size], sem.at[0]))
                out.append((w_up.at[q, :, lo : lo + size], buf.at[:, size : 2 * size], sem.at[1]))
        return out

    def fetch(ph, q, r=0):
        for c in tile_copies(ph, q, r):
            pltpu.make_async_copy(*c).start()

    def fetch_pair(ph, i):
        kind = stream[ph][0]
        if kind == 'gate_up':
            fetch(ph, jnp.int32(i // gu_pairs), i % gu_pairs)
        else:
            fetch(ph, jnp.int32(i))

    def arrive(ph, q, r=0):
        for c in tile_copies(ph, q, r):
            pltpu.make_async_copy(*c).wait()

    ahead = SLOTS - 1

    def next_pair(ph, q):
        n = stream[ph][2]

        @pl.when(q + ahead < n)
        def _():
            fetch(ph, q + ahead)

        if ph + 1 < len(stream):
            for k in range(ahead):
                @pl.when(q == n - ahead + k)
                def _(k=k):
                    fetch_pair(ph + 1, k)

    def next_pair_gu(ph, e, r):
        if r + ahead < gu_pairs:
            fetch(ph, e, r + ahead)
            return
        over = r + ahead - gu_pairs
        step, pos = 1 + over // gu_pairs, over % gu_pairs

        @pl.when(e + step < local_n)
        def _():
            fetch(ph, e + step, pos)

        for k in range(ahead):
            @pl.when(e * gu_pairs + r + ahead == stream[ph][2] + k)
            def _(k=k):
                fetch_pair(ph + 1, k)

    def own(m):
        return x_a if m == 0 else land.at[m, me]

    def rows_half(ref, hf):
        return ref.at[hf * half_n : (hf + 1) * half_n]

    def g_partner(m):
        return remote(own(m), land.at[m, me], gather_send.at[m, 0], gather_recv.at[m, 0], partner)

    def g_near(m, d, hf):
        k = 1 + 2 * d + hf
        return remote(
            rows_half(own(m), hf), rows_half(land.at[m, me], hf), gather_send.at[m, k], gather_recv.at[m, k], sides[d]
        )

    def g_forward(m, d):
        block = rows_half(land.at[m, sides[1 - d]], d)
        return remote(block, block, gather_send.at[m, 5 + d], gather_recv.at[m, 5 + d], sides[d])

    def g_pass(m, d):
        block = land.at[m, sides[1 - d]]
        return remote(block, block, gather_send.at[m, 7 + d], gather_recv.at[m, 7 + d], partner)

    def g_pass_far(m, d):
        block = rows_half(land.at[m, far], d)
        return remote(block, block, gather_send.at[m, 9 + d], gather_recv.at[m, 9 + d], partner)

    def gather_start(m):
        g_partner(m).start()
        for step in range(2):
            for d in range(2):
                g_near(m, d, d if step == 0 else 1 - d).start()

    def gather_forward(m):
        for d in range(2):
            g_near(m, d, d).wait_recv()
            g_forward(m, d).start()

    def gather_pass(m):
        for d in range(2):
            g_near(m, d, 1 - d).wait_recv()
            g_pass(m, d).start()

    def gather_near_done(m):
        g_partner(m).wait_recv()
        for d in range(2):
            g_pass(m, d).wait_recv()

    def gather_pass_far(m):
        for d in range(2):
            g_forward(m, d).wait_recv()
            g_pass_far(m, d).start()

    def gather_done(m):
        for d in range(2):
            g_pass_far(m, d).wait_recv()
        g_partner(m).wait_send()
        for d in range(2):
            g_near(m, d, 0).wait_send()
            g_near(m, d, 1).wait_send()
            g_forward(m, d).wait_send()
            g_pass(m, d).wait_send()
            g_pass_far(m, d).wait_send()

    def source_at(k):
        kk = div(k, 2)
        off = kk + div(kk, 2) - 2 * div(kk, 3)
        return 2 * rem(chip + off, n_chips) + rem(k, 2)

    class load:
        def __init__(self, m, k):
            self.copies = [
                pltpu.make_async_copy(
                    land.at[m, source_at(k), :, j * cols : (j + 1) * cols],
                    expert_out.at[CHUNKS * rem(k, 2) + j, 0:tok_n],
                    load_sem.at[rem(k, 2), j],
                )
                for j in range(CHUNKS)
            ]

        def start(self):
            for c in self.copies:
                c.start()

        def wait(self):
            for c in self.copies:
                c.wait()

    def dispatch(m, lo, hi):
        load(m, jnp.int32(lo)).start()

        def body(k, carry):
            @pl.when(k + 1 < hi)
            def _():
                load(m, k + 1).start()

            s, slot = source_at(k), rem(k, 2)
            load(m, k).wait()
            rank = table[s, m, 0:local_n]
            slots = lax.broadcasted_iota(jnp.int32, (capacity, tok_n), 0).astype(F32)
            pick = jnp.concatenate(
                [jnp.where(rank[e : e + 1] == slots, 1.0, 0.0).astype(BF16) for e in range(local_n)], axis=0
            )
            for j in range(CHUNKS):
                part = slice(j * cols, (j + 1) * cols)
                got = jnp.dot(pick, expert_out[CHUNKS * slot + j, 0:tok_n], preferred_element_type=F32).astype(BF16)
                for e in range(local_n):
                    rows[e, pl.ds(pl.multiple_of(s * capacity, capacity), capacity), part] = got[
                        e * capacity : (e + 1) * capacity
                    ]
            return carry

        lax.fori_loop(jnp.int32(lo), jnp.int32(hi), body, 0)

    def make_mixer(m):
        lane = lax.broadcasted_iota(jnp.int32, (2 * local_n, n_slots), 1)
        line = lax.broadcasted_iota(jnp.int32, (2 * local_n, n_slots), 0)

        def spread(first):
            low = (line - first) * capacity
            inside = (line >= first) & (line < first + local_n) & (lane >= low) & (lane < low + capacity)
            return jnp.where(inside, 1.0, 0.0).astype(BF16)

        spread_rank, spread_gate = spread(0), spread(local_n)
        at = lax.broadcasted_iota(jnp.int32, (tok_n, n_slots), 1)
        base = jnp.zeros_like(at)
        for e in range(1, local_n):
            base = base + jnp.where(at >= e * capacity, capacity, 0)
        at = (at - base).astype(F32)

        def body(s, carry):
            value = table[s, m]
            hi = value.astype(BF16)
            rest = value - hi.astype(F32)
            mid = rest.astype(BF16)
            low = (rest - mid.astype(F32)).astype(BF16)

            def turn(v, e):
                return lax.dot_general(v, e, (((0,), (0,)), ((), ())), preferred_element_type=F32)

            here = turn(hi, spread_rank) == at
            for k, v in enumerate((hi, mid, low)):
                mixer[s, k * tok_n : (k + 1) * tok_n] = jnp.where(here, turn(v, spread_gate), 0.0).astype(BF16)
            return carry

        lax.fori_loop(jnp.int32(0), jnp.int32(n_devs), body, 0)

    def r_pair(n):
        return remote(partial.at[1 - core], pair.at[n], pair_send.at[n], pair_recv.at[n], partner)

    def r_far(n, d):
        return remote(pair.at[n, chip_far, d], transit.at[n, d], far_send.at[n, d], far_recv.at[n, d], sides[d])

    def r_near(n, d, hf):
        return remote(
            pair.at[n, chip_side[d], hf], near.at[n, d, hf], near_send.at[n, d, hf], near_recv.at[n, d, hf], sides[d]
        )

    def own_rows(m, n):
        return pltpu.make_async_copy(
            land.at[m, me, :, sl(n * cols, cols)], own_stage.at[n], own_sem.at[n]
        )

    def out_copy(m, n):
        return pltpu.make_async_copy(
            out_stage.at[n], (out_a, out_b)[m].at[:, sl(n * cols, cols)], stage_sem.at[n]
        )

    def back_pair(n):
        r_pair(n).start()

    def back_far(n):
        r_pair(n).wait()

        def body(k, carry):
            for hf in range(2):
                pair[n, k, hf] += partial[core, k, hf]
            return carry

        lax.fori_loop(jnp.int32(0), jnp.int32(n_chips), body, 0)
        for d in range(2):
            r_far(n, d).start()
        for d in range(2):
            r_near(n, d, 1 - d).start()

    def back_near(m, n):
        for d in range(2):
            r_far(n, d).wait_recv()
            pair[n, chip_side[d], d] += transit[n, d]
            r_near(n, d, d).start()
        own_rows(m, n).start()

    def back_out(m, n):
        for d in range(2):
            r_far(n, d).wait_send()
            for hf in range(2):
                r_near(n, d, hf).wait()
        own_rows(m, n).wait()
        if m == 1:
            out_copy(0, n).wait()
        for hf in range(2):
            part = slice(hf * half, (hf + 1) * half)
            total = pair[n, chip, hf] + near[n, 0, hf] + near[n, 1, hf]
            out_stage[n, :, part] = (own_stage[n, :, part].astype(F32) + total).astype(BF16)
        out_copy(m, n).start()

    for k in range(ahead):
        fetch_pair(0, k)
    barrier = pltpu.get_barrier_semaphore()
    for k in range(1, n_devs):
        pl.semaphore_signal(
            barrier, inc=1, device_id={'ep': rem(me + k, n_devs)}, device_id_type=pl.DeviceIdType.MESH
        )
    attn_in = pltpu.make_async_copy(attn_b, rows.at[0, 0:tok_n], load_sem.at[0, 0])
    h_in = pltpu.make_async_copy(h_b, rows.at[1, 0:tok_n], load_sem.at[1, 0])
    x_in = pltpu.make_async_copy(x_a, rows.at[3, 0:tok_n], own_sem.at[0])
    attn_in.start()
    h_in.start()
    x_in.start()
    pl.semaphore_wait(barrier, n_devs - 1)

    def m_send(k):
        to = rem(me + k, n_devs)
        return remote(meta.at[to], table.at[me], meta_send.at[k], meta_recv.at[k], to)

    gather_start(0)
    n_experts = n_devs * local_n
    before = jnp.where(
        lax.broadcasted_iota(jnp.int32, (tok_n, tok_n), 0) < lax.broadcasted_iota(jnp.int32, (tok_n, tok_n), 1), 1.0, 0.0
    ).astype(BF16)
    ids = lax.broadcasted_iota(jnp.int32, (n_experts, tok_n), 0)
    for m, (route, gate) in enumerate(((route_a, gate_a), (route_b, gate_b))):
        chosen = jnp.zeros((n_experts, tok_n), F32)
        gates = jnp.zeros((n_experts, tok_n), F32)
        for j in range(route.shape[0]):
            hit = route[j : j + 1] == ids
            chosen = jnp.where(hit, 1.0, chosen)
            gates = jnp.where(hit, gate[j : j + 1], gates)
        rank = jnp.dot(chosen.astype(BF16), before, preferred_element_type=F32)
        rank = jnp.where(chosen > 0.5, rank, -1.0)
        for d in range(n_devs):
            meta[d, m, 0:local_n] = rank[d * local_n : (d + 1) * local_n]
            meta[d, m, local_n : 2 * local_n] = gates[d * local_n : (d + 1) * local_n]
    for k in range(1, n_devs):
        m_send(k).start()
    table[me] = meta[me]
    x_in.wait()
    x_put = pltpu.make_async_copy(rows.at[3, 0:tok_n], land.at[0, me], own_sem.at[0])
    x_put.start()
    attn_in.wait()
    h_in.wait()

    def proj_pair(q, carry):
        arrive(0, q)
        next_pair(0, q)
        slot = slot_of(0, q)
        for k in range(2):
            part = sl((2 * q + k) * cols, cols)
            got = jnp.dot(rows[0, 0:tok_n], wbuf[slot, k, :, 0:cols], preferred_element_type=F32).astype(BF16)
            rows[2, 0:tok_n, part] = (rows[1, 0:tok_n, part].astype(F32) + got.astype(F32)).astype(BF16)
        return carry

    lax.fori_loop(jnp.int32(0), jnp.int32(stream[0][2]), proj_pair, 0)
    mid_put = pltpu.make_async_copy(rows.at[2, 0:tok_n], land.at[1, me], own_sem.at[1])
    mid_put.start()

    def qkv_copy(j):
        return pltpu.make_async_copy(
            out_stage.at[rem(j, CHUNKS)], qkv.at[:, sl(j * cols, cols)], stage_sem.at[rem(j, CHUNKS)]
        )

    def qkv_pair(q, carry):
        arrive(1, q)
        next_pair(1, q)
        slot = slot_of(1, q)
        for k in range(2):
            j = 2 * q + k

            @pl.when(j >= CHUNKS)
            def _(j=j):
                qkv_copy(j - CHUNKS).wait()

        for k in range(2):
            j = 2 * q + k
            got = jnp.dot(rows[1, 0:tok_n], wbuf[slot, k, :, 0:cols], preferred_element_type=F32)
            out_stage[rem(j, CHUNKS)] = got.astype(BF16)
        for k in range(2):
            qkv_copy(2 * q + k).start()

        @pl.when(q == stream[1][2] // 2)
        def _():
            gather_forward(0)

        return carry

    lax.fori_loop(jnp.int32(0), jnp.int32(stream[1][2]), qkv_pair, 0)
    x_put.wait()
    mid_put.wait()
    for j in range(2 * stream[1][2] - CHUNKS, 2 * stream[1][2]):
        qkv_copy(jnp.int32(j)).wait()
    for k in range(1, n_devs):
        m_send(k).wait()
    make_mixer(0)
    gather_pass(0)
    gather_start(1)
    gather_near_done(0)

    for m in range(2):
        dispatch(m, 0, n_devs - 2)
        if m == 0:
            gather_pass_far(0)
            gather_done(0)
        dispatch(m, n_devs - 2, n_devs)
        if m == 1:
            make_mixer(1)
            back_far(jnp.int32(CHUNKS - 1))
            back_near(0, jnp.int32(1))

        def gu_expert(e, carry, m=m):
            ph = 2 + 2 * m
            for r in range(gu_pairs):
                arrive(ph, e, r)
                next_pair_gu(ph, e, r)
                slot = slot_of(ph, e * gu_pairs + r)
                for k in range(2):
                    t = 2 * r + k
                    if t < n_full:
                        g = jnp.dot(rows[e], wbuf[slot, k, :, 0:WIDE], preferred_element_type=F32)
                        u = jnp.dot(rows[e], wbuf[slot, k, :, WIDE : 2 * WIDE], preferred_element_type=F32)
                        hidden[e, :, t * WIDE : (t + 1) * WIDE] = (jax.nn.silu(g) * u).astype(BF16)
                    else:
                        gu = jnp.dot(rows[e], wbuf[slot, k, :, 0 : 2 * tail], preferred_element_type=F32)
                        hidden[e, :, n_full * WIDE : ff] = (
                            jax.nn.silu(gu[:, 0:tail]) * gu[:, tail : 2 * tail]
                        ).astype(BF16)

            if m == 0:
                events = {2: [lambda: gather_forward(1)], 4: [lambda: gather_pass(1)]}
            else:
                events = {
                    1: [lambda: back_near(0, jnp.int32(2))],
                    3: [lambda: back_out(0, jnp.int32(0))],
                    4: [lambda: back_near(0, jnp.int32(3))],
                    5: [lambda: back_out(0, jnp.int32(1))],
                    6: [lambda: back_out(0, jnp.int32(2))],
                    7: [lambda: back_out(0, jnp.int32(3))],
                }
            for at, steps in events.items():
                def run(steps=steps):
                    for step in steps:
                        step()
                pl.when(e == at)(run)
            return carry

        lax.fori_loop(jnp.int32(0), jnp.int32(local_n), gu_expert, 0)
        if m == 0:
            gather_pass_far(1)
        else:
            for dev in (partner, right, left):
                pl.semaphore_signal(credit, inc=1, device_id={'ep': dev}, device_id_type=pl.DeviceIdType.MESH)

        def down_chunk(n, carry, m=m):
            ph = 3 + 2 * m

            def pair_of(r, carry):
                q = n * (local_n // 2) + r
                arrive(ph, q)
                next_pair(ph, q)
                slot = slot_of(ph, q)
                for k in range(2):
                    e = 2 * r + k
                    y = jnp.dot(hidden[e], wbuf[slot, k, 0:ff, 0:cols], preferred_element_type=F32).astype(BF16)
                    expert_out[:, pl.ds(pl.multiple_of(e * capacity, capacity), capacity), :] = y.reshape(
                        n_devs, capacity, cols
                    )

                @pl.when((r == 1) & (n == 2))
                def _():
                    back_near(m, jnp.int32(0))

                @pl.when((r == 2) & (n >= 1))
                def _():
                    back_far(n - 1)

                return carry

            lax.fori_loop(jnp.int32(0), jnp.int32(local_n // 2), pair_of, 0)

            def mix(r, carry):
                for k in range(2):
                    for hf in range(2):
                        ys = expert_out[2 * r + k, :, hf * half : (hf + 1) * half]
                        got = jnp.dot(mixer[2 * r + k], ys, preferred_element_type=F32)
                        partial[k, r, hf] = got[0:tok_n] + got[tok_n : 2 * tok_n] + got[2 * tok_n : 3 * tok_n]
                return carry

            lax.fori_loop(jnp.int32(0), jnp.int32(n_devs // 2), mix, 0)
            if m == 1:
                @pl.when(n == 0)
                def _():
                    pl.semaphore_wait(credit, 3)

            back_pair(n)
            return carry

        lax.fori_loop(jnp.int32(0), jnp.int32(CHUNKS), down_chunk, 0)
        if m == 0:
            gather_near_done(1)
            gather_done(1)

    back_near(1, jnp.int32(1))
    back_far(jnp.int32(CHUNKS - 1))
    back_near(1, jnp.int32(2))
    back_out(1, jnp.int32(0))
    back_near(1, jnp.int32(3))
    for n in range(1, CHUNKS):
        back_out(1, jnp.int32(n))
    for n in range(CHUNKS):
        out_copy(1, jnp.int32(n)).wait()


def hand_over_kernel(*refs):
    ins, outs, bufs, sems = refs[0:3], refs[3:6], refs[6:9], refs[9]
    pieces = sems.shape[2]
    size = ins[0].shape[0] // pieces

    def move(src, dst, i, p, way):
        at = pl.ds(p * size, size)
        return pltpu.make_async_copy(src.at[at], dst.at[at], sems.at[way, i, p])

    todo = [(i, p) for i in range(3) for p in range(pieces)]
    for i, p in todo:
        move(ins[i], bufs[i], i, p, 0).start()
    for i, p in todo:
        move(ins[i], bufs[i], i, p, 0).wait()
        move(bufs[i], outs[i], i, p, 1).start()
    for i, p in todo:
        move(bufs[i], outs[i], i, p, 1).wait()


def hand_over(arrays):
    any_spec = pl.BlockSpec(memory_space=pl.ANY)
    return pl.pallas_call(
        hand_over_kernel,
        in_specs=[any_spec] * 3,
        out_specs=[any_spec] * 3,
        out_shape=[jax.ShapeDtypeStruct(a.shape, a.dtype) for a in arrays],
        scratch_shapes=[pltpu.VMEM(a.shape, a.dtype) for a in arrays] + [pltpu.SemaphoreType.DMA((2, 3, 4))],
        compiler_params=pltpu.CompilerParams(vmem_limit_bytes=VMEM_LIMIT),
        name="hand_over",
    )(*arrays)


def solution(mesh):
    n_devs = mesh.shape['ep']

    def local_step(x_a, route_a, gate_a, h_b, attn_b, route_b, gate_b, w_qkv, w_o, w_gate, w_up, w_down):
        tok_n, dim = x_a.shape
        top_k = route_a.shape[1]
        local_n, _, ff = w_gate.shape
        n_experts = local_n * n_devs
        capacity = min(tok_n, 2 * ((tok_n * top_k + n_experts - 1) // n_experts))
        row_n, n_slots, cols = n_devs * capacity, local_n * capacity, dim // CHUNKS
        half, n_chips = cols // 2, n_devs // 2

        any_spec = pl.BlockSpec(memory_space=pl.ANY)
        dma = pltpu.SemaphoreType.DMA

        def body(*refs):
            moe_kernel(capacity, *refs)

        flops = 2 * (6 * local_n * row_n * dim * ff + 8 * n_devs * n_slots * tok_n * dim) + 2 * tok_n * dim * 4 * dim
        out_a, out_b, qkv_b, _ = pl.pallas_call(
            body,
            in_specs=[any_spec] * 3 + [pl.BlockSpec(memory_space=pltpu.VMEM)] * 4 + [any_spec] * 5,
            out_specs=[any_spec] * 4,
            out_shape=[
                jax.ShapeDtypeStruct((tok_n, dim), BF16),
                jax.ShapeDtypeStruct((tok_n, dim), BF16),
                jax.ShapeDtypeStruct((tok_n, w_qkv.shape[1]), BF16),
                jax.ShapeDtypeStruct((2, n_devs, tok_n, dim), BF16),
            ],
            scratch_shapes=[
                pltpu.VMEM((SLOTS, 2, dim, max(cols, 2 * WIDE)), BF16),
                pltpu.VMEM((local_n, row_n, dim), BF16),
                pltpu.VMEM((local_n, row_n, ff), BF16),
                pltpu.VMEM((n_devs, 2, 2 * local_n, tok_n), F32),
                pltpu.VMEM((n_devs, n_slots, cols), BF16),
                pltpu.VMEM((n_devs, 3 * tok_n, n_slots), BF16),
                pltpu.VMEM((2, n_chips, 2, tok_n, half), F32),
                pltpu.VMEM((CHUNKS, n_chips, 2, tok_n, half), F32),
                pltpu.VMEM((CHUNKS, 2, tok_n, half), F32),
                pltpu.VMEM((CHUNKS, 2, 2, tok_n, half), F32),
                pltpu.VMEM((CHUNKS, tok_n, cols), BF16),
                pltpu.VMEM((CHUNKS, tok_n, cols), BF16),
                pltpu.VMEM((n_devs, 2, 2 * local_n, tok_n), F32),
                dma((SLOTS, 2, 2)),
                dma((2, 11)),
                dma((2, 11)),
                dma((n_devs,)),
                dma((n_devs,)),
                dma((2, CHUNKS)),
                dma((CHUNKS,)),
                dma((CHUNKS,)),
                dma((CHUNKS,)),
                dma((CHUNKS,)),
                dma((CHUNKS, 2)),
                dma((CHUNKS, 2)),
                dma((CHUNKS, 2, 2)),
                dma((CHUNKS, 2, 2)),
                pltpu.SemaphoreType.REGULAR,
            ],
            compiler_params=pltpu.CompilerParams(
                collective_id=0, has_side_effects=True, vmem_limit_bytes=VMEM_LIMIT
            ),
            cost_estimate=pl.CostEstimate(flops=flops, bytes_accessed=400_000_000, transcendentals=0),
            name="moe_step",
        )(x_a, h_b, attn_b, route_a.T, gate_a.T, route_b.T, gate_b.T, w_qkv, w_o, w_gate, w_up, w_down)
        return tuple(hand_over((out_a, out_b, qkv_b)))

    row_spec = P(('dp', 'ep'), None)
    full_spec = P(None, None)
    expert_spec = P('ep', None, None)
    return jax.shard_map(
        local_step,
        mesh=mesh,
        in_specs=(row_spec, row_spec, row_spec, row_spec, row_spec, row_spec, row_spec, full_spec, full_spec, expert_spec, expert_spec, expert_spec),
        out_specs=(row_spec, row_spec, row_spec),
        check_vma=False,
    )
```

```python
import jax
import jax.numpy as jnp
from jax import lax
from jax.experimental import pallas as pl
from jax.experimental.pallas import tpu as pltpu
from jax.sharding import PartitionSpec as P

F32 = jnp.float32
BF16 = jnp.bfloat16
VMEM_LIMIT = 67_000_000
WIDE = 256
SLOTS = 3
CHUNKS = 4


def rem(a, b):
    return lax.rem(a, jnp.int32(b))


def div(a, b):
    return lax.div(a, jnp.int32(b))


def moe_kernel(
    capacity,
    x_a, h_b, attn_b, route_a, gate_a, route_b, gate_b, w_qkv, w_o, w_gate, w_up, w_down,
    out, qkv, land,
    wbuf, rows, hidden, meta, expert_out, mixer, partial, pair, transit, near, out_stage, own_stage, table,
    w_sem, gather_send, gather_recv, meta_send, meta_recv, load_sem, stage_sem, own_sem,
    pair_send, pair_recv, far_send, far_recv, near_send, near_recv, ring_credit, pair_credit,
):
    n_devs = land.shape[1]
    n_chips = n_devs // 2
    tok_n, dim = x_a.shape
    half_n = tok_n // 2
    local_n, row_n, ff = hidden.shape
    n_slots = local_n * capacity
    cols = dim // CHUNKS
    half = cols // 2
    n_full, tail = ff // WIDE, ff % WIDE
    gu_tiles = n_full + 1

    me = lax.axis_index('ep')
    chip, core = div(me, 2), rem(me, 2)
    partner = me + 1 - 2 * core
    right, left = rem(me + 2, n_devs), rem(me + n_devs - 2, n_devs)
    sides = (right, left)
    chip_right, chip_left, chip_far = rem(chip + 1, n_chips), rem(chip + n_chips - 1, n_chips), rem(chip + 2, n_chips)
    chip_side = (chip_right, chip_left)
    far = 2 * chip_far + core

    def remote(src, dst, send, recv, dev):
        return pltpu.make_async_remote_copy(
            src_ref=src, dst_ref=dst, send_sem=send, recv_sem=recv, device_id={'ep': dev},
            device_id_type=pl.DeviceIdType.MESH,
        )

    def sl(start, size):
        return pl.ds(pl.multiple_of(start, size), size)

    pairs_of = {'proj': CHUNKS // 2, 'qkv': qkv.shape[1] // cols // 2, 'down': CHUNKS * local_n // 2}
    gu_pairs = gu_tiles // 2
    pairs_of['gate_up'] = local_n * gu_pairs
    stream, total = [], 0
    for kind in ('proj', 'qkv') + ('gate_up', 'down') * 3:
        stream.append((kind, total, pairs_of[kind]))
        total += pairs_of[kind]

    def slot_of(ph, q):
        return rem(q + stream[ph][1], SLOTS)

    def tile_copies(ph, q, r=0):
        kind = stream[ph][0]
        slot = slot_of(ph, q * gu_pairs + r if kind == 'gate_up' else q)
        out = []
        for k in range(2):
            buf, sem = wbuf.at[slot, k], w_sem.at[slot, k]
            if kind in ('proj', 'qkv'):
                w = w_o if kind == 'proj' else w_qkv
                out.append((w.at[:, sl((2 * q + k) * cols, cols)], buf.at[:, 0:cols], sem.at[0]))
            elif kind == 'down':
                n, e = div(q, local_n // 2), rem(q, local_n // 2) * 2 + k
                out.append((w_down.at[e, :, sl(n * cols, cols)], buf.at[0:ff, 0:cols], sem.at[0]))
            else:
                t = 2 * r + k
                lo, size = t * WIDE, WIDE if t < n_full else tail
                out.append((w_gate.at[q, :, lo : lo + size], buf.at[:, 0:size], sem.at[0]))
                out.append((w_up.at[q, :, lo : lo + size], buf.at[:, size : 2 * size], sem.at[1]))
        return out

    def fetch(ph, q, r=0):
        for c in tile_copies(ph, q, r):
            pltpu.make_async_copy(*c).start()

    def fetch_pair(ph, i):
        kind = stream[ph][0]
        if kind == 'gate_up':
            fetch(ph, jnp.int32(i // gu_pairs), i % gu_pairs)
        else:
            fetch(ph, jnp.int32(i))

    def arrive(ph, q, r=0):
        for c in tile_copies(ph, q, r):
            pltpu.make_async_copy(*c).wait()

    ahead = SLOTS - 1

    def next_pair(ph, q):
        n = stream[ph][2]

        @pl.when(q + ahead < n)
        def _():
            fetch(ph, q + ahead)

        if ph + 1 < len(stream):
            for k in range(ahead):
                @pl.when(q == n - ahead + k)
                def _(k=k):
                    fetch_pair(ph + 1, k)

    def next_pair_gu(ph, e, r):
        if r + ahead < gu_pairs:
            fetch(ph, e, r + ahead)
            return
        over = r + ahead - gu_pairs
        step, pos = 1 + over // gu_pairs, over % gu_pairs

        @pl.when(e + step < local_n)
        def _():
            fetch(ph, e + step, pos)

        for k in range(ahead):
            @pl.when(e * gu_pairs + r + ahead == stream[ph][2] + k)
            def _(k=k):
                fetch_pair(ph + 1, k)

    def own(m):
        return x_a if m == 0 else land.at[m, me]

    def rows_half(ref, hf):
        return ref.at[hf * half_n : (hf + 1) * half_n]

    def g_partner(m):
        return remote(own(m), land.at[m, me], gather_send.at[m, 0], gather_recv.at[m, 0], partner)

    def g_near(m, d, hf):
        k = 1 + 2 * d + hf
        return remote(
            rows_half(own(m), hf), rows_half(land.at[m, me], hf), gather_send.at[m, k], gather_recv.at[m, k], sides[d]
        )

    def g_forward(m, d):
        block = rows_half(land.at[m, sides[1 - d]], d)
        return remote(block, block, gather_send.at[m, 5 + d], gather_recv.at[m, 5 + d], sides[d])

    def g_pass(m, d):
        block = land.at[m, sides[1 - d]]
        return remote(block, block, gather_send.at[m, 7 + d], gather_recv.at[m, 7 + d], partner)

    def g_pass_far(m, d):
        block = rows_half(land.at[m, far], d)
        return remote(block, block, gather_send.at[m, 9 + d], gather_recv.at[m, 9 + d], partner)

    def gather_start(m):
        g_partner(m).start()
        for step in range(2):
            for d in range(2):
                g_near(m, d, d if step == 0 else 1 - d).start()

    def gather_forward(m):
        for d in range(2):
            g_near(m, d, d).wait_recv()
            g_forward(m, d).start()

    def gather_pass(m):
        for d in range(2):
            g_near(m, d, 1 - d).wait_recv()
            g_pass(m, d).start()

    def gather_pass_far(m):
        for d in range(2):
            g_forward(m, d).wait_recv()
            g_pass_far(m, d).start()

    def gather_from_partner(m):
        g_partner(m).wait_recv()
        for d in range(2):
            g_pass(m, d).wait_recv()
            g_pass_far(m, d).wait_recv()

    def gather_sent(m):
        g_partner(m).wait_send()
        for d in range(2):
            g_near(m, d, 0).wait_send()
            g_near(m, d, 1).wait_send()
            g_forward(m, d).wait_send()
            g_pass(m, d).wait_send()
            g_pass_far(m, d).wait_send()

    def on_core(c, *steps):
        @pl.when(core == c)
        def _():
            for step in steps:
                step()

    n_pass = 3
    sources = [n_chips, 2 * n_chips, n_chips]
    members = [(0,), (0, 1), (1,)]

    def batch_at(ps, t):
        return div(t, n_chips) if ps == 1 else jnp.int32(ps // 2)

    def core_at(ps, t):
        return 1 - div(t, n_chips) if ps == 1 else jnp.int32(ps // 2)

    def source_at(ps, t):
        return 2 * rem(t, n_chips) + core_at(ps, t)

    def my_batch(ps):
        return 1 - core if ps == 1 else jnp.int32(ps // 2)

    class load:
        def __init__(self, ps, k):
            self.copies = [
                pltpu.make_async_copy(
                    land.at[batch_at(ps, k), source_at(ps, k), :, j * cols : (j + 1) * cols],
                    expert_out.at[CHUNKS * rem(k, 2) + j, 0:tok_n],
                    load_sem.at[rem(k, 2), j],
                )
                for j in range(CHUNKS)
            ]

        def start(self):
            for c in self.copies:
                c.start()

        def wait(self):
            for c in self.copies:
                c.wait()

    def dispatch(ps):
        hi = sources[ps]
        load(ps, jnp.int32(0)).start()

        def body(k, carry):
            @pl.when(k + 1 < hi)
            def _():
                load(ps, k + 1).start()

            slot = rem(k, 2)
            load(ps, k).wait()
            rank = table[source_at(ps, k), batch_at(ps, k), 0:local_n]
            slots = lax.broadcasted_iota(jnp.int32, (capacity, tok_n), 0).astype(F32)
            pick = jnp.concatenate(
                [jnp.where(rank[e : e + 1] == slots, 1.0, 0.0).astype(BF16) for e in range(local_n)], axis=0
            )
            for j in range(CHUNKS):
                part = slice(j * cols, (j + 1) * cols)
                got = jnp.dot(pick, expert_out[CHUNKS * slot + j, 0:tok_n], preferred_element_type=F32).astype(BF16)
                for e in range(local_n):
                    rows[e, pl.ds(pl.multiple_of(k * capacity, capacity), capacity), part] = got[
                        e * capacity : (e + 1) * capacity
                    ]
            return carry

        lax.fori_loop(jnp.int32(0), jnp.int32(hi), body, 0)

    def make_mixer(ps):
        lane = lax.broadcasted_iota(jnp.int32, (2 * local_n, n_slots), 1)
        line = lax.broadcasted_iota(jnp.int32, (2 * local_n, n_slots), 0)

        def spread(first):
            low = (line - first) * capacity
            inside = (line >= first) & (line < first + local_n) & (lane >= low) & (lane < low + capacity)
            return jnp.where(inside, 1.0, 0.0).astype(BF16)

        spread_rank, spread_gate = spread(0), spread(local_n)
        at = lax.broadcasted_iota(jnp.int32, (tok_n, n_slots), 1)
        base = jnp.zeros_like(at)
        for e in range(1, local_n):
            base = base + jnp.where(at >= e * capacity, capacity, 0)
        at = (at - base).astype(F32)

        def body(s, carry):
            value = table[source_at(ps, s), batch_at(ps, s)]
            hi = value.astype(BF16)
            rest = value - hi.astype(F32)
            mid = rest.astype(BF16)
            low = (rest - mid.astype(F32)).astype(BF16)

            def turn(v, e):
                return lax.dot_general(v, e, (((0,), (0,)), ((), ())), preferred_element_type=F32)

            here = turn(hi, spread_rank) == at
            for k, v in enumerate((hi, mid, low)):
                mixer[s, k * tok_n : (k + 1) * tok_n] = jnp.where(here, turn(v, spread_gate), 0.0).astype(BF16)
            return carry

        lax.fori_loop(jnp.int32(0), jnp.int32(sources[ps]), body, 0)

    def r_pair(n):
        return remote(partial.at[1 - core], pair.at[n], pair_send.at[n], pair_recv.at[n], partner)

    def r_far(n, d):
        return remote(pair.at[n, chip_far, d], transit.at[n, d], far_send.at[n, d], far_recv.at[n, d], sides[d])

    def r_near(n, d, hf):
        return remote(
            pair.at[n, chip_side[d], hf], near.at[n, d, hf], near_send.at[n, d, hf], near_recv.at[n, d, hf], sides[d]
        )

    def own_rows(m, n):
        return pltpu.make_async_copy(
            land.at[m, me, :, sl(n * cols, cols)], own_stage.at[n], own_sem.at[n]
        )

    def out_copy(m, n):
        return pltpu.make_async_copy(out_stage.at[n], out.at[m, :, sl(n * cols, cols)], stage_sem.at[n])

    def by_role(ps, ring, feeder):
        if ps == 1:
            ring()
            feeder()
        else:
            on_core(ps // 2, ring)
            on_core(1 - ps // 2, feeder)

    def back_pair(ps, n):
        by_role(ps, lambda: None, lambda: r_pair(n).start())

    def back_far(ps, n):
        def ring():
            r_pair(n).wait_recv()

            def body(k, carry):
                for hf in range(2):
                    pair[n, k, hf] += partial[core, k, hf]
                return carry

            lax.fori_loop(jnp.int32(0), jnp.int32(n_chips), body, 0)
            for d in range(2):
                r_far(n, d).start()
            for d in range(2):
                r_near(n, d, 1 - d).start()

        by_role(ps, ring, lambda: r_pair(n).wait_send())

    def back_near(ps, n):
        def ring():
            for d in range(2):
                r_far(n, d).wait_recv()
                pair[n, chip_side[d], d] += transit[n, d]
                r_near(n, d, d).start()
            own_rows(my_batch(ps), n).start()

        by_role(ps, ring, lambda: None)

    def back_out(ps, n):
        def ring():
            m = my_batch(ps)
            for d in range(2):
                r_far(n, d).wait_send()
                for hf in range(2):
                    r_near(n, d, hf).wait()
            own_rows(m, n).wait()
            if ps > 0:
                @pl.when(m == 1)
                def _():
                    out_copy(0, n).wait()
            for hf in range(2):
                part = slice(hf * half, (hf + 1) * half)
                total = pair[n, chip, hf] + near[n, 0, hf] + near[n, 1, hf]
                out_stage[n, :, part] = (own_stage[n, :, part].astype(F32) + total).astype(BF16)
            out_copy(m, n).start()

        by_role(ps, ring, lambda: None)

    def give_credit():
        for dev in (right, left):
            pl.semaphore_signal(ring_credit, inc=1, device_id={'ep': dev}, device_id_type=pl.DeviceIdType.MESH)
        pl.semaphore_signal(pair_credit, inc=1, device_id={'ep': partner}, device_id_type=pl.DeviceIdType.MESH)

    for k in range(ahead):
        fetch_pair(0, k)
    barrier = pltpu.get_barrier_semaphore()
    for k in range(1, n_devs):
        pl.semaphore_signal(
            barrier, inc=1, device_id={'ep': rem(me + k, n_devs)}, device_id_type=pl.DeviceIdType.MESH
        )
    attn_in = pltpu.make_async_copy(attn_b, rows.at[0, 0:tok_n], load_sem.at[0, 0])
    h_in = pltpu.make_async_copy(h_b, rows.at[1, 0:tok_n], load_sem.at[1, 0])
    x_in = pltpu.make_async_copy(x_a, rows.at[3, 0:tok_n], own_sem.at[0])
    attn_in.start()
    h_in.start()
    x_in.start()
    pl.semaphore_wait(barrier, n_devs - 1)

    def m_send(k):
        to = rem(me + k, n_devs)
        return remote(meta.at[to], table.at[me], meta_send.at[k], meta_recv.at[k], to)

    on_core(0, lambda: gather_start(0))
    n_experts = n_devs * local_n
    before = jnp.where(
        lax.broadcasted_iota(jnp.int32, (tok_n, tok_n), 0) < lax.broadcasted_iota(jnp.int32, (tok_n, tok_n), 1), 1.0, 0.0
    ).astype(BF16)
    ids = lax.broadcasted_iota(jnp.int32, (n_experts, tok_n), 0)
    for m, (route, gate) in enumerate(((route_a, gate_a), (route_b, gate_b))):
        chosen = jnp.zeros((n_experts, tok_n), F32)
        gates = jnp.zeros((n_experts, tok_n), F32)
        for j in range(route.shape[0]):
            hit = route[j : j + 1] == ids
            chosen = jnp.where(hit, 1.0, chosen)
            gates = jnp.where(hit, gate[j : j + 1], gates)
        rank = jnp.dot(chosen.astype(BF16), before, preferred_element_type=F32)
        rank = jnp.where(chosen > 0.5, rank, -1.0)
        for d in range(n_devs):
            meta[d, m, 0:local_n] = rank[d * local_n : (d + 1) * local_n]
            meta[d, m, local_n : 2 * local_n] = gates[d * local_n : (d + 1) * local_n]
    for k in range(1, n_devs):
        m_send(k).start()
    table[me] = meta[me]
    x_in.wait()
    x_put = pltpu.make_async_copy(rows.at[3, 0:tok_n], land.at[0, me], own_sem.at[0])
    x_put.start()
    attn_in.wait()
    h_in.wait()

    def proj_pair(q, carry):
        arrive(0, q)
        next_pair(0, q)
        slot = slot_of(0, q)
        for k in range(2):
            part = sl((2 * q + k) * cols, cols)
            got = jnp.dot(rows[0, 0:tok_n], wbuf[slot, k, :, 0:cols], preferred_element_type=F32).astype(BF16)
            rows[2, 0:tok_n, part] = (rows[1, 0:tok_n, part].astype(F32) + got.astype(F32)).astype(BF16)
        return carry

    lax.fori_loop(jnp.int32(0), jnp.int32(stream[0][2]), proj_pair, 0)
    mid_put = pltpu.make_async_copy(rows.at[2, 0:tok_n], land.at[1, me], own_sem.at[1])
    mid_put.start()

    def qkv_copy(j):
        return pltpu.make_async_copy(
            out_stage.at[rem(j, CHUNKS)], qkv.at[:, sl(j * cols, cols)], stage_sem.at[rem(j, CHUNKS)]
        )

    def qkv_pair(q, carry):
        arrive(1, q)
        next_pair(1, q)
        slot = slot_of(1, q)
        for k in range(2):
            j = 2 * q + k

            @pl.when(j >= CHUNKS)
            def _(j=j):
                qkv_copy(j - CHUNKS).wait()

        for k in range(2):
            j = 2 * q + k
            got = jnp.dot(rows[1, 0:tok_n], wbuf[slot, k, :, 0:cols], preferred_element_type=F32)
            out_stage[rem(j, CHUNKS)] = got.astype(BF16)
        for k in range(2):
            qkv_copy(2 * q + k).start()

        @pl.when(q == stream[1][2] // 2)
        def _():
            on_core(0, lambda: gather_forward(0))

        return carry

    lax.fori_loop(jnp.int32(0), jnp.int32(stream[1][2]), qkv_pair, 0)
    x_put.wait()
    mid_put.wait()
    for j in range(2 * stream[1][2] - CHUNKS, 2 * stream[1][2]):
        qkv_copy(jnp.int32(j)).wait()
    for k in range(1, n_devs):
        m_send(k).wait()
    on_core(0, lambda: gather_pass(0), lambda: gather_pass_far(0), lambda: gather_start(1))
    on_core(1, lambda: gather_from_partner(0), lambda: gather_start(0))
    i32 = jnp.int32
    last = CHUNKS - 1

    for ps in range(n_pass):
        n_src = sources[ps]
        taken = n_src * capacity
        if ps == 1:
            on_core(0, lambda: gather_from_partner(0))
            on_core(1, lambda: gather_from_partner(1))
        if ps == 2:
            on_core(0, lambda: gather_from_partner(1), lambda: gather_sent(0), lambda: gather_sent(1))
            on_core(1, lambda: gather_sent(0), lambda: gather_sent(1))
        dispatch(ps)
        if ps > 0:
            back_far(ps - 1, i32(last))
            back_near(ps - 1, i32(1))
        make_mixer(ps)

        gu_events = [
            {
                2: lambda: (on_core(0, lambda: gather_forward(1)), on_core(1, lambda: gather_forward(0))),
                4: lambda: (
                    on_core(0, lambda: gather_pass(1)),
                    on_core(1, lambda: gather_pass(0), lambda: gather_start(1)),
                ),
            },
            {
                0: lambda: (back_near(0, i32(2)), on_core(1, lambda: gather_forward(1))),
                1: lambda: (back_near(0, i32(3)), on_core(1, lambda: gather_pass(1))),
                3: lambda: back_out(0, i32(0)),
                4: lambda: (back_out(0, i32(1)), on_core(1, lambda: gather_pass_far(1))),
                5: lambda: back_out(0, i32(2)),
                6: lambda: (back_out(0, i32(3)), on_core(0, give_credit)),
            },
            {
                1: lambda: back_near(1, i32(2)),
                3: lambda: back_out(1, i32(0)),
                4: lambda: back_near(1, i32(3)),
                5: lambda: back_out(1, i32(1)),
                6: lambda: back_out(1, i32(2)),
            },
        ][ps]

        def gu_expert(e, carry, ps=ps, taken=taken, gu_events=gu_events):
            ph = 2 + 2 * ps
            for r in range(gu_pairs):
                arrive(ph, e, r)
                next_pair_gu(ph, e, r)
                slot = slot_of(ph, e * gu_pairs + r)
                for k in range(2):
                    t = 2 * r + k
                    x = rows[e, 0:taken]
                    if t < n_full:
                        g = jnp.dot(x, wbuf[slot, k, :, 0:WIDE], preferred_element_type=F32)
                        u = jnp.dot(x, wbuf[slot, k, :, WIDE : 2 * WIDE], preferred_element_type=F32)
                        hidden[e, 0:taken, t * WIDE : (t + 1) * WIDE] = (jax.nn.silu(g) * u).astype(BF16)
                    else:
                        gu = jnp.dot(x, wbuf[slot, k, :, 0 : 2 * tail], preferred_element_type=F32)
                        hidden[e, 0:taken, n_full * WIDE : ff] = (
                            jax.nn.silu(gu[:, 0:tail]) * gu[:, tail : 2 * tail]
                        ).astype(BF16)
            for at, step in gu_events.items():
                pl.when(e == at)(lambda step=step: (step(), None)[1])
            return carry

        lax.fori_loop(i32(0), i32(local_n), gu_expert, 0)

        def down_chunk(n, carry, ps=ps, n_src=n_src, taken=taken):
            ph = 3 + 2 * ps
            final = local_n // 2 - 1

            def pair_of(r, carry):
                q = n * (local_n // 2) + r
                arrive(ph, q)
                next_pair(ph, q)
                slot = slot_of(ph, q)
                for k in range(2):
                    e = 2 * r + k
                    y = jnp.dot(hidden[e, 0:taken], wbuf[slot, k, 0:ff, 0:cols], preferred_element_type=F32)
                    expert_out[0:n_src, pl.ds(pl.multiple_of(e * capacity, capacity), capacity), :] = (
                        y.astype(BF16).reshape(n_src, capacity, cols)
                    )

                if ps == 0:
                    @pl.when((r == final) & (n == 0))
                    def _():
                        on_core(0, lambda: gather_pass_far(1))
                        on_core(1, lambda: gather_pass_far(0))

                if ps == 2:
                    @pl.when((r == 1) & (n == 0))
                    def _():
                        back_out(1, i32(last))
                        on_core(1, give_credit)

                @pl.when((r == final) & (n == 2))
                def _():
                    back_near(ps, i32(0))

                @pl.when((r == (final - 1 if ps == 1 else final)) & (n >= 1))
                def _():
                    back_far(ps, n - 1)

                return carry

            lax.fori_loop(i32(0), i32(local_n // 2), pair_of, 0)

            def mix(r, carry):
                for k in range(2):
                    t = 2 * r + k
                    for hf in range(2):
                        ys = expert_out[t, :, hf * half : (hf + 1) * half]
                        got = jnp.dot(mixer[t], ys, preferred_element_type=F32)
                        partial[core_at(ps, t), rem(t, n_chips), hf] = (
                            got[0:tok_n] + got[tok_n : 2 * tok_n] + got[2 * tok_n : 3 * tok_n]
                        )
                return carry

            lax.fori_loop(i32(0), i32(n_src // 2), mix, 0)
            if ps > 0:
                @pl.when(n == 0)
                def _():
                    on_core(ps - 1, lambda: pl.semaphore_wait(ring_credit, 2))
                    on_core(2 - ps, lambda: pl.semaphore_wait(pair_credit, 1))

            back_pair(ps, n)
            return carry

        lax.fori_loop(i32(0), i32(CHUNKS), down_chunk, 0)

    back_far(2, i32(last))
    back_near(2, i32(1))
    back_near(2, i32(2))
    back_out(2, i32(0))
    back_near(2, i32(3))
    for n in range(1, CHUNKS):
        back_out(2, i32(n))
    for n in range(CHUNKS):
        out_copy(1, i32(n)).wait()


def hand_over_kernel(both, qkv, out_a, out_b, out_qkv, *scratch):
    ins, outs, bufs, sems = (both.at[0], both.at[1], qkv), (out_a, out_b, out_qkv), scratch[0:3], scratch[3]
    pieces = sems.shape[2]
    size = qkv.shape[0] // pieces

    def move(src, dst, i, p, way):
        at = pl.ds(p * size, size)
        return pltpu.make_async_copy(src.at[at], dst.at[at], sems.at[way, i, p])

    todo = [(i, p) for i in range(3) for p in range(pieces)]
    for i, p in todo:
        move(ins[i], bufs[i], i, p, 0).start()
    for i, p in todo:
        move(ins[i], bufs[i], i, p, 0).wait()
        move(bufs[i], outs[i], i, p, 1).start()
    for i, p in todo:
        move(bufs[i], outs[i], i, p, 1).wait()


def hand_over(both, qkv):
    any_spec = pl.BlockSpec(memory_space=pl.ANY)
    results = [jax.ShapeDtypeStruct(both.shape[1:], both.dtype)] * 2 + [jax.ShapeDtypeStruct(qkv.shape, qkv.dtype)]
    return pl.pallas_call(
        hand_over_kernel,
        in_specs=[any_spec] * 2,
        out_specs=[any_spec] * 3,
        out_shape=results,
        scratch_shapes=[pltpu.VMEM(a.shape, a.dtype) for a in results] + [pltpu.SemaphoreType.DMA((2, 3, 4))],
        compiler_params=pltpu.CompilerParams(vmem_limit_bytes=VMEM_LIMIT),
        name="hand_over",
    )(both, qkv)


def solution(mesh):
    n_devs = mesh.shape['ep']

    def local_step(x_a, route_a, gate_a, h_b, attn_b, route_b, gate_b, w_qkv, w_o, w_gate, w_up, w_down):
        tok_n, dim = x_a.shape
        top_k = route_a.shape[1]
        local_n, _, ff = w_gate.shape
        n_experts = local_n * n_devs
        capacity = min(tok_n, 2 * ((tok_n * top_k + n_experts - 1) // n_experts))
        row_n, n_slots, cols = n_devs * capacity, local_n * capacity, dim // CHUNKS
        half, n_chips = cols // 2, n_devs // 2

        any_spec = pl.BlockSpec(memory_space=pl.ANY)
        dma = pltpu.SemaphoreType.DMA

        def body(*refs):
            moe_kernel(capacity, *refs)

        flops = 2 * (6 * local_n * row_n * dim * ff + 8 * n_devs * n_slots * tok_n * dim) + 2 * tok_n * dim * 4 * dim
        both, qkv_b, _ = pl.pallas_call(
            body,
            in_specs=[any_spec] * 3 + [pl.BlockSpec(memory_space=pltpu.VMEM)] * 4 + [any_spec] * 5,
            out_specs=[any_spec] * 3,
            out_shape=[
                jax.ShapeDtypeStruct((2, tok_n, dim), BF16),
                jax.ShapeDtypeStruct((tok_n, w_qkv.shape[1]), BF16),
                jax.ShapeDtypeStruct((2, n_devs, tok_n, dim), BF16),
            ],
            scratch_shapes=[
                pltpu.VMEM((SLOTS, 2, dim, max(cols, 2 * WIDE)), BF16),
                pltpu.VMEM((local_n, row_n, dim), BF16),
                pltpu.VMEM((local_n, row_n, ff), BF16),
                pltpu.VMEM((n_devs, 2, 2 * local_n, tok_n), F32),
                pltpu.VMEM((n_devs, n_slots, cols), BF16),
                pltpu.VMEM((n_devs, 3 * tok_n, n_slots), BF16),
                pltpu.VMEM((2, n_chips, 2, tok_n, half), F32),
                pltpu.VMEM((CHUNKS, n_chips, 2, tok_n, half), F32),
                pltpu.VMEM((CHUNKS, 2, tok_n, half), F32),
                pltpu.VMEM((CHUNKS, 2, 2, tok_n, half), F32),
                pltpu.VMEM((CHUNKS, tok_n, cols), BF16),
                pltpu.VMEM((CHUNKS, tok_n, cols), BF16),
                pltpu.VMEM((n_devs, 2, 2 * local_n, tok_n), F32),
                dma((SLOTS, 2, 2)),
                dma((2, 11)),
                dma((2, 11)),
                dma((n_devs,)),
                dma((n_devs,)),
                dma((2, CHUNKS)),
                dma((CHUNKS,)),
                dma((CHUNKS,)),
                dma((CHUNKS,)),
                dma((CHUNKS,)),
                dma((CHUNKS, 2)),
                dma((CHUNKS, 2)),
                dma((CHUNKS, 2, 2)),
                dma((CHUNKS, 2, 2)),
                pltpu.SemaphoreType.REGULAR,
                pltpu.SemaphoreType.REGULAR,
            ],
            compiler_params=pltpu.CompilerParams(
                collective_id=0, has_side_effects=True, vmem_limit_bytes=VMEM_LIMIT
            ),
            cost_estimate=pl.CostEstimate(flops=flops, bytes_accessed=400_000_000, transcendentals=0),
            name="moe_step",
        )(x_a, h_b, attn_b, route_a.T, gate_a.T, route_b.T, gate_b.T, w_qkv, w_o, w_gate, w_up, w_down)
        return tuple(hand_over(both, qkv_b))

    row_spec = P(('dp', 'ep'), None)
    full_spec = P(None, None)
    expert_spec = P('ep', None, None)
    return jax.shard_map(
        local_step,
        mesh=mesh,
        in_specs=(row_spec, row_spec, row_spec, row_spec, row_spec, row_spec, row_spec, full_spec, full_spec, expert_spec, expert_spec, expert_spec),
        out_specs=(row_spec, row_spec, row_spec),
        check_vma=False,
    )
```

```python
import jax
import jax.numpy as jnp
from jax import lax
from jax.experimental import pallas as pl
from jax.experimental.pallas import tpu as pltpu
from jax.sharding import PartitionSpec as P

F32 = jnp.float32
BF16 = jnp.bfloat16
VMEM_LIMIT = 67_000_000
WIDE = 256
SLOTS = 3
CHUNKS = 4


def rem(a, b):
    return lax.rem(a, jnp.int32(b))


def div(a, b):
    return lax.div(a, jnp.int32(b))


def moe_kernel(
    capacity,
    x_a, h_b, attn_b, route_a, gate_a, route_b, gate_b, w_qkv, w_o, w_gate, w_up, w_down,
    out, qkv, land,
    wbuf, rows, hidden, meta, src_rows, mixer, partial, pair, transit, near, out_stage, own_stage, table,
    w_sem, gather_send, gather_recv, meta_send, meta_recv, load_sem, stage_sem, own_sem,
    pair_send, pair_recv, far_send, far_recv, near_send, near_recv, ring_credit, pair_credit,
):
    n_devs = land.shape[1]
    n_chips = n_devs // 2
    tok_n, dim = x_a.shape
    half_n = tok_n // 2
    local_n, row_n, ff = hidden.shape
    n_slots = local_n * capacity
    cols = dim // CHUNKS
    half = cols // 2
    n_full, tail = ff // WIDE, ff % WIDE
    gu_tiles = n_full + 1

    me = lax.axis_index('ep')
    chip, core = div(me, 2), rem(me, 2)
    partner = me + 1 - 2 * core
    right, left = rem(me + 2, n_devs), rem(me + n_devs - 2, n_devs)
    sides = (right, left)
    chip_right, chip_left, chip_far = rem(chip + 1, n_chips), rem(chip + n_chips - 1, n_chips), rem(chip + 2, n_chips)
    chip_side = (chip_right, chip_left)
    far = 2 * chip_far + core

    def remote(src, dst, send, recv, dev):
        return pltpu.make_async_remote_copy(
            src_ref=src, dst_ref=dst, send_sem=send, recv_sem=recv, device_id={'ep': dev},
            device_id_type=pl.DeviceIdType.MESH,
        )

    def sl(start, size):
        return pl.ds(pl.multiple_of(start, size), size)

    pairs_of = {'proj': CHUNKS // 2, 'qkv': qkv.shape[1] // cols // 2, 'down': CHUNKS * local_n // 2}
    gu_pairs = gu_tiles // 2
    pairs_of['gate_up'] = local_n * gu_pairs
    stream, total = [], 0
    for kind in ('proj', 'qkv') + ('gate_up', 'down') * 3:
        stream.append((kind, total, pairs_of[kind]))
        total += pairs_of[kind]

    def slot_of(ph, q):
        return rem(q + stream[ph][1], SLOTS)

    def tile_copies(ph, q, r=0):
        kind = stream[ph][0]
        slot = slot_of(ph, q * gu_pairs + r if kind == 'gate_up' else q)
        out = []
        for k in range(2):
            buf, sem = wbuf.at[slot, k], w_sem.at[slot, k]
            if kind in ('proj', 'qkv'):
                w = w_o if kind == 'proj' else w_qkv
                out.append((w.at[:, sl((2 * q + k) * cols, cols)], buf.at[:, 0:cols], sem.at[0]))
            elif kind == 'down':
                e, n = div(q, CHUNKS // 2), rem(q, CHUNKS // 2) * 2 + k
                out.append((w_down.at[e, :, sl(n * cols, cols)], buf.at[0:ff, 0:cols], sem.at[0]))
            else:
                t = 2 * r + k
                lo, size = t * WIDE, WIDE if t < n_full else tail
                out.append((w_gate.at[q, :, lo : lo + size], buf.at[:, 0:size], sem.at[0]))
                out.append((w_up.at[q, :, lo : lo + size], buf.at[:, size : 2 * size], sem.at[1]))
        return out

    def fetch(ph, q, r=0):
        for c in tile_copies(ph, q, r):
            pltpu.make_async_copy(*c).start()

    def fetch_pair(ph, i):
        kind = stream[ph][0]
        if kind == 'gate_up':
            fetch(ph, jnp.int32(i // gu_pairs), i % gu_pairs)
        else:
            fetch(ph, jnp.int32(i))

    def arrive(ph, q, r=0):
        for c in tile_copies(ph, q, r):
            pltpu.make_async_copy(*c).wait()

    ahead = SLOTS - 1

    def next_pair(ph, q):
        n = stream[ph][2]

        @pl.when(q + ahead < n)
        def _():
            fetch(ph, q + ahead)

        if ph + 1 < len(stream):
            for k in range(ahead):
                @pl.when(q == n - ahead + k)
                def _(k=k):
                    fetch_pair(ph + 1, k)

    def next_pair_gu(ph, e, r):
        if r + ahead < gu_pairs:
            fetch(ph, e, r + ahead)
            return
        over = r + ahead - gu_pairs
        step, pos = 1 + over // gu_pairs, over % gu_pairs

        @pl.when(e + step < local_n)
        def _():
            fetch(ph, e + step, pos)

        for k in range(ahead):
            @pl.when(e * gu_pairs + r + ahead == stream[ph][2] + k)
            def _(k=k):
                fetch_pair(ph + 1, k)

    def own(m):
        return x_a if m == 0 else land.at[m, me]

    def rows_half(ref, hf):
        return ref.at[hf * half_n : (hf + 1) * half_n]

    def g_partner(m):
        return remote(own(m), land.at[m, me], gather_send.at[m, 0], gather_recv.at[m, 0], partner)

    def g_near(m, d, hf):
        k = 1 + 2 * d + hf
        return remote(
            rows_half(own(m), hf), rows_half(land.at[m, me], hf), gather_send.at[m, k], gather_recv.at[m, k], sides[d]
        )

    def g_forward(m, d):
        block = rows_half(land.at[m, sides[1 - d]], d)
        return remote(block, block, gather_send.at[m, 5 + d], gather_recv.at[m, 5 + d], sides[d])

    def g_pass(m, d):
        block = land.at[m, sides[1 - d]]
        return remote(block, block, gather_send.at[m, 7 + d], gather_recv.at[m, 7 + d], partner)

    def g_pass_far(m, d):
        block = rows_half(land.at[m, far], d)
        return remote(block, block, gather_send.at[m, 9 + d], gather_recv.at[m, 9 + d], partner)

    def gather_start(m):
        g_partner(m).start()
        for step in range(2):
            for d in range(2):
                g_near(m, d, d if step == 0 else 1 - d).start()

    def gather_forward(m):
        for d in range(2):
            g_near(m, d, d).wait_recv()
            g_forward(m, d).start()

    def gather_pass(m):
        for d in range(2):
            g_near(m, d, 1 - d).wait_recv()
            g_pass(m, d).start()

    def gather_pass_far(m):
        for d in range(2):
            g_forward(m, d).wait_recv()
            g_pass_far(m, d).start()

    def gather_from_partner(m):
        g_partner(m).wait_recv()
        for d in range(2):
            g_pass(m, d).wait_recv()
            g_pass_far(m, d).wait_recv()

    def gather_sent(m):
        g_partner(m).wait_send()
        for d in range(2):
            g_near(m, d, 0).wait_send()
            g_near(m, d, 1).wait_send()
            g_forward(m, d).wait_send()
            g_pass(m, d).wait_send()
            g_pass_far(m, d).wait_send()

    def on_core(c, *steps):
        @pl.when(core == c)
        def _():
            for step in steps:
                step()

    n_pass = 3
    sources = [n_chips, 2 * n_chips, n_chips]
    members = [(0,), (0, 1), (1,)]

    def batch_at(ps, t):
        return div(t, n_chips) if ps == 1 else jnp.int32(ps // 2)

    def core_at(ps, t):
        return 1 - div(t, n_chips) if ps == 1 else jnp.int32(ps // 2)

    def source_at(ps, t):
        return 2 * rem(t, n_chips) + core_at(ps, t)

    def my_batch(ps):
        return 1 - core if ps == 1 else jnp.int32(ps // 2)

    def load(ps, k):
        slot = rem(k, 2)
        return pltpu.make_async_copy(land.at[batch_at(ps, k), source_at(ps, k)], src_rows.at[slot], load_sem.at[slot])

    def dispatch(ps):
        hi = sources[ps]
        load(ps, jnp.int32(0)).start()

        def body(k, carry):
            @pl.when(k + 1 < hi)
            def _():
                load(ps, k + 1).start()

            slot = rem(k, 2)
            load(ps, k).wait()
            rank = table[source_at(ps, k), batch_at(ps, k), 0:local_n]
            slots = lax.broadcasted_iota(jnp.int32, (capacity, tok_n), 0).astype(F32)
            pick = jnp.concatenate(
                [jnp.where(rank[e : e + 1] == slots, 1.0, 0.0).astype(BF16) for e in range(local_n)], axis=0
            )
            for j in range(CHUNKS):
                part = slice(j * cols, (j + 1) * cols)
                got = jnp.dot(pick, src_rows[slot, :, part], preferred_element_type=F32).astype(BF16)
                for e in range(local_n):
                    rows[e, pl.ds(pl.multiple_of(k * capacity, capacity), capacity), part] = got[
                        e * capacity : (e + 1) * capacity
                    ]
            return carry

        lax.fori_loop(jnp.int32(0), jnp.int32(hi), body, 0)

    def make_mixer(ps):
        lane = lax.broadcasted_iota(jnp.int32, (2 * local_n, n_slots), 1)
        line = lax.broadcasted_iota(jnp.int32, (2 * local_n, n_slots), 0)

        def spread(first):
            low = (line - first) * capacity
            inside = (line >= first) & (line < first + local_n) & (lane >= low) & (lane < low + capacity)
            return jnp.where(inside, 1.0, 0.0).astype(BF16)

        spread_rank, spread_gate = spread(0), spread(local_n)
        at = lax.broadcasted_iota(jnp.int32, (tok_n, n_slots), 1)
        base = jnp.zeros_like(at)
        for e in range(1, local_n):
            base = base + jnp.where(at >= e * capacity, capacity, 0)
        at = (at - base).astype(F32)

        def body(s, carry):
            value = table[source_at(ps, s), batch_at(ps, s)]
            hi = value.astype(BF16)
            rest = value - hi.astype(F32)
            mid = rest.astype(BF16)
            low = (rest - mid.astype(F32)).astype(BF16)

            def turn(v, e):
                return lax.dot_general(v, e, (((0,), (0,)), ((), ())), preferred_element_type=F32)

            here = turn(hi, spread_rank) == at
            for k, v in enumerate((hi, mid, low)):
                mixer[s, k * tok_n : (k + 1) * tok_n] = jnp.where(here, turn(v, spread_gate), 0.0).astype(BF16)
            return carry

        lax.fori_loop(jnp.int32(0), jnp.int32(sources[ps]), body, 0)

    def r_pair(n):
        return remote(partial.at[1 + rem(n, 2)], pair.at[n], pair_send.at[n], pair_recv.at[n], partner)

    def r_far(n, d):
        return remote(pair.at[n, chip_far, d], transit.at[n, d], far_send.at[n, d], far_recv.at[n, d], sides[d])

    def r_near(n, d, hf):
        return remote(
            pair.at[n, chip_side[d], hf], near.at[n, d, hf], near_send.at[n, d, hf], near_recv.at[n, d, hf], sides[d]
        )

    def own_rows(m, n):
        return pltpu.make_async_copy(
            land.at[m, me, :, sl(n * cols, cols)], own_stage.at[n], own_sem.at[n]
        )

    def out_copy(m, n):
        return pltpu.make_async_copy(out_stage.at[n], out.at[m, :, sl(n * cols, cols)], stage_sem.at[n])

    def by_role(ps, ring, feeder):
        if ps == 1:
            ring()
            feeder()
        else:
            on_core(ps // 2, ring)
            on_core(1 - ps // 2, feeder)

    def back_pair(ps, n):
        by_role(ps, lambda: None, lambda: r_pair(n).start())

    def back_far(ps, n):
        def ring():
            r_pair(n).wait_recv()

            def body(k, carry):
                for hf in range(2):
                    pair[n, k, hf] += partial[0, k, hf]
                return carry

            lax.fori_loop(jnp.int32(0), jnp.int32(n_chips), body, 0)
            for d in range(2):
                r_far(n, d).start()
            for d in range(2):
                r_near(n, d, 1 - d).start()

        by_role(ps, ring, lambda: None)

    def back_given(ps, n):
        by_role(ps, lambda: None, lambda: r_pair(n).wait_send())

    def back_near(ps, n):
        def ring():
            for d in range(2):
                r_far(n, d).wait_recv()
                pair[n, chip_side[d], d] += transit[n, d]
                r_near(n, d, d).start()
            own_rows(my_batch(ps), n).start()

        by_role(ps, ring, lambda: None)

    def back_out(ps, n):
        def ring():
            m = my_batch(ps)
            for d in range(2):
                r_far(n, d).wait_send()
                for hf in range(2):
                    r_near(n, d, hf).wait()
            own_rows(m, n).wait()
            if ps > 0:
                @pl.when(m == 1)
                def _():
                    out_copy(0, n).wait()
            for hf in range(2):
                part = slice(hf * half, (hf + 1) * half)
                total = pair[n, chip, hf] + near[n, 0, hf] + near[n, 1, hf]
                out_stage[n, :, part] = (own_stage[n, :, part].astype(F32) + total).astype(BF16)
            out_copy(m, n).start()

        by_role(ps, ring, lambda: None)

    def give_credit():
        for dev in (right, left):
            pl.semaphore_signal(ring_credit, inc=1, device_id={'ep': dev}, device_id_type=pl.DeviceIdType.MESH)
        pl.semaphore_signal(pair_credit, inc=1, device_id={'ep': partner}, device_id_type=pl.DeviceIdType.MESH)

    for k in range(ahead):
        fetch_pair(0, k)
    barrier = pltpu.get_barrier_semaphore()
    for k in range(1, n_devs):
        pl.semaphore_signal(
            barrier, inc=1, device_id={'ep': rem(me + k, n_devs)}, device_id_type=pl.DeviceIdType.MESH
        )
    attn_in = pltpu.make_async_copy(attn_b, rows.at[0, 0:tok_n], load_sem.at[0])
    h_in = pltpu.make_async_copy(h_b, rows.at[1, 0:tok_n], load_sem.at[1])
    x_in = pltpu.make_async_copy(x_a, rows.at[3, 0:tok_n], own_sem.at[0])
    attn_in.start()
    h_in.start()
    x_in.start()
    pl.semaphore_wait(barrier, n_devs - 1)

    def m_send(k):
        to = rem(me + k, n_devs)
        return remote(meta.at[to], table.at[me], meta_send.at[k], meta_recv.at[k], to)

    on_core(0, lambda: gather_start(0))
    n_experts = n_devs * local_n
    before = jnp.where(
        lax.broadcasted_iota(jnp.int32, (tok_n, tok_n), 0) < lax.broadcasted_iota(jnp.int32, (tok_n, tok_n), 1), 1.0, 0.0
    ).astype(BF16)
    ids = lax.broadcasted_iota(jnp.int32, (n_experts, tok_n), 0)
    for m, (route, gate) in enumerate(((route_a, gate_a), (route_b, gate_b))):
        chosen = jnp.zeros((n_experts, tok_n), F32)
        gates = jnp.zeros((n_experts, tok_n), F32)
        for j in range(route.shape[0]):
            hit = route[j : j + 1] == ids
            chosen = jnp.where(hit, 1.0, chosen)
            gates = jnp.where(hit, gate[j : j + 1], gates)
        rank = jnp.dot(chosen.astype(BF16), before, preferred_element_type=F32)
        rank = jnp.where(chosen > 0.5, rank, -1.0)
        for d in range(n_devs):
            meta[d, m, 0:local_n] = rank[d * local_n : (d + 1) * local_n]
            meta[d, m, local_n : 2 * local_n] = gates[d * local_n : (d + 1) * local_n]
    for k in range(1, n_devs):
        m_send(k).start()
    table[me] = meta[me]
    x_in.wait()
    x_put = pltpu.make_async_copy(rows.at[3, 0:tok_n], land.at[0, me], own_sem.at[0])
    x_put.start()
    attn_in.wait()
    h_in.wait()

    def proj_pair(q, carry):
        arrive(0, q)
        next_pair(0, q)
        slot = slot_of(0, q)
        for k in range(2):
            part = sl((2 * q + k) * cols, cols)
            got = jnp.dot(rows[0, 0:tok_n], wbuf[slot, k, :, 0:cols], preferred_element_type=F32).astype(BF16)
            rows[2, 0:tok_n, part] = (rows[1, 0:tok_n, part].astype(F32) + got.astype(F32)).astype(BF16)
        return carry

    lax.fori_loop(jnp.int32(0), jnp.int32(stream[0][2]), proj_pair, 0)
    mid_put = pltpu.make_async_copy(rows.at[2, 0:tok_n], land.at[1, me], own_sem.at[1])
    mid_put.start()

    def qkv_copy(j):
        return pltpu.make_async_copy(
            out_stage.at[rem(j, CHUNKS)], qkv.at[:, sl(j * cols, cols)], stage_sem.at[rem(j, CHUNKS)]
        )

    def qkv_pair(q, carry):
        arrive(1, q)
        next_pair(1, q)
        slot = slot_of(1, q)
        for k in range(2):
            j = 2 * q + k

            @pl.when(j >= CHUNKS)
            def _(j=j):
                qkv_copy(j - CHUNKS).wait()

        for k in range(2):
            j = 2 * q + k
            got = jnp.dot(rows[1, 0:tok_n], wbuf[slot, k, :, 0:cols], preferred_element_type=F32)
            out_stage[rem(j, CHUNKS)] = got.astype(BF16)
        for k in range(2):
            qkv_copy(2 * q + k).start()

        @pl.when(q == stream[1][2] // 2)
        def _():
            on_core(0, lambda: gather_forward(0))

        return carry

    lax.fori_loop(jnp.int32(0), jnp.int32(stream[1][2]), qkv_pair, 0)
    x_put.wait()
    mid_put.wait()
    for j in range(2 * stream[1][2] - CHUNKS, 2 * stream[1][2]):
        qkv_copy(jnp.int32(j)).wait()
    for k in range(1, n_devs):
        m_send(k).wait()
    on_core(0, lambda: gather_pass(0), lambda: gather_pass_far(0), lambda: gather_start(1))
    on_core(1, lambda: gather_from_partner(0), lambda: gather_start(0))
    i32 = jnp.int32
    last = CHUNKS - 1

    for ps in range(n_pass):
        n_src = sources[ps]
        taken = n_src * capacity
        if ps == 1:
            on_core(0, lambda: gather_from_partner(0))
            on_core(1, lambda: gather_from_partner(1))
        if ps == 2:
            on_core(0, lambda: gather_from_partner(1), lambda: gather_sent(0), lambda: gather_sent(1))
            on_core(1, lambda: gather_sent(0), lambda: gather_sent(1))
        dispatch(ps)
        if ps > 0:
            back_far(ps - 1, i32(last))
        if ps == 1:
            back_near(0, i32(0))
        make_mixer(ps)

        gu_events = [
            {
                2: lambda: (on_core(0, lambda: gather_forward(1)), on_core(1, lambda: gather_forward(0))),
                4: lambda: (
                    on_core(0, lambda: gather_pass(1)),
                    on_core(1, lambda: gather_pass(0), lambda: gather_start(1)),
                ),
            },
            {
                0: lambda: (back_near(0, i32(1)), on_core(1, lambda: gather_forward(1))),
                1: lambda: (back_near(0, i32(2)), on_core(1, lambda: gather_pass(1))),
                2: lambda: back_near(0, i32(3)),
                3: lambda: back_out(0, i32(0)),
                4: lambda: (back_out(0, i32(1)), on_core(1, lambda: gather_pass_far(1))),
                5: lambda: back_out(0, i32(2)),
                6: lambda: (back_out(0, i32(3)), on_core(0, give_credit)),
            },
            {
                0: lambda: back_near(1, i32(1)),
                3: lambda: back_near(1, i32(2)),
                5: lambda: back_out(1, i32(0)),
                7: lambda: back_near(1, i32(3)),
            },
        ][ps]

        def gu_expert(e, carry, ps=ps, taken=taken, gu_events=gu_events):
            ph = 2 + 2 * ps
            for r in range(gu_pairs):
                arrive(ph, e, r)
                next_pair_gu(ph, e, r)
                slot = slot_of(ph, e * gu_pairs + r)
                for k in range(2):
                    t = 2 * r + k
                    x = rows[e, 0:taken]
                    if t < n_full:
                        g = jnp.dot(x, wbuf[slot, k, :, 0:WIDE], preferred_element_type=F32)
                        u = jnp.dot(x, wbuf[slot, k, :, WIDE : 2 * WIDE], preferred_element_type=F32)
                        hidden[e, 0:taken, t * WIDE : (t + 1) * WIDE] = (jax.nn.silu(g) * u).astype(BF16)
                    else:
                        gu = jnp.dot(x, wbuf[slot, k, :, 0 : 2 * tail], preferred_element_type=F32)
                        hidden[e, 0:taken, n_full * WIDE : ff] = (
                            jax.nn.silu(gu[:, 0:tail]) * gu[:, tail : 2 * tail]
                        ).astype(BF16)
            for at, step in gu_events.items():
                pl.when(e == at)(lambda step=step: (step(), None)[1])
            return carry

        lax.fori_loop(i32(0), i32(local_n), gu_expert, 0)

        def down_pair(q, carry, ps=ps, taken=taken):
            ph = 3 + 2 * ps
            arrive(ph, q)
            next_pair(ph, q)
            slot = slot_of(ph, q)
            e, first = div(q, CHUNKS // 2), rem(q, CHUNKS // 2) * 2
            for k in range(2):
                y = jnp.dot(hidden[e, 0:taken], wbuf[slot, k, 0:ff, 0:cols], preferred_element_type=F32)
                rows[e, 0:taken, sl((first + k) * cols, cols)] = y.astype(BF16)

            if ps == 0:
                @pl.when(q == 3)
                def _():
                    on_core(0, lambda: gather_pass_far(1))
                    on_core(1, lambda: gather_pass_far(0))

            if ps == 2:
                for at, n in ((2, 1), (6, 2)):
                    @pl.when(q == at)
                    def _(n=n):
                        back_out(1, i32(n))

            return carry

        lax.fori_loop(i32(0), i32(CHUNKS // 2 * local_n), down_pair, 0)
        if ps == 2:
            back_out(1, i32(last))
            on_core(1, give_credit)
        if ps > 0:
            on_core(ps - 1, lambda: pl.semaphore_wait(ring_credit, 2))
            on_core(2 - ps, lambda: pl.semaphore_wait(pair_credit, 1))

        def mix_chunk(n, carry, ps=ps, n_src=n_src):
            def mix(lo, where):
                def body(r, carry):
                    for k in range(2):
                        t = rem(lo + 2 * r + k, n_src)
                        here = pl.ds(pl.multiple_of(t * capacity, capacity), capacity)
                        for hf in range(2):
                            at = sl(n * cols + hf * half, half)
                            ys = jnp.concatenate([rows[e, here, at] for e in range(local_n)], axis=0)
                            got = jnp.dot(mixer[t], ys, preferred_element_type=F32)
                            partial[where, rem(t, n_chips), hf] = (
                                got[0:tok_n] + got[tok_n : 2 * tok_n] + got[2 * tok_n : 3 * tok_n]
                            )
                    return carry

                lax.fori_loop(i32(0), i32(n_chips // 2), body, 0)

            @pl.when(n >= 2)
            def _():
                back_given(ps, n - 2)

            def follow():
                @pl.when(n >= 1)
                def _():
                    back_far(ps, n - 1)

            if ps == 1:
                mix(n_chips * core, 1 + rem(n, 2))
                back_pair(ps, n)
                follow()
                mix(n_chips * (1 - core), 0)
            else:
                follow()
                mine = 1 - (ps // 2 - core) * (ps // 2 - core)
                mix(i32(0), (1 - mine) * (1 + rem(n, 2)))
                back_pair(ps, n)
            return carry

        lax.fori_loop(i32(0), i32(CHUNKS), mix_chunk, 0)
        for n in range(CHUNKS - 2, CHUNKS):
            back_given(ps, i32(n))
        if ps == 1:
            back_near(ps, i32(0))

    back_far(2, i32(last))
    back_near(2, i32(0))
    back_near(2, i32(1))
    back_near(2, i32(2))
    back_out(2, i32(0))
    back_near(2, i32(3))
    for n in range(1, CHUNKS):
        back_out(2, i32(n))
    for n in range(CHUNKS):
        out_copy(1, i32(n)).wait()


def hand_over_kernel(both, qkv, out_a, out_b, out_qkv, *scratch):
    ins, outs, bufs, sems = (both.at[0], both.at[1], qkv), (out_a, out_b, out_qkv), scratch[0:3], scratch[3]
    pieces = sems.shape[2]
    size = qkv.shape[0] // pieces

    def move(src, dst, i, p, way):
        at = pl.ds(p * size, size)
        return pltpu.make_async_copy(src.at[at], dst.at[at], sems.at[way, i, p])

    todo = [(i, p) for i in range(3) for p in range(pieces)]
    for i, p in todo:
        move(ins[i], bufs[i], i, p, 0).start()
    for i, p in todo:
        move(ins[i], bufs[i], i, p, 0).wait()
        move(bufs[i], outs[i], i, p, 1).start()
    for i, p in todo:
        move(bufs[i], outs[i], i, p, 1).wait()


def hand_over(both, qkv):
    any_spec = pl.BlockSpec(memory_space=pl.ANY)
    results = [jax.ShapeDtypeStruct(both.shape[1:], both.dtype)] * 2 + [jax.ShapeDtypeStruct(qkv.shape, qkv.dtype)]
    return pl.pallas_call(
        hand_over_kernel,
        in_specs=[any_spec] * 2,
        out_specs=[any_spec] * 3,
        out_shape=results,
        scratch_shapes=[pltpu.VMEM(a.shape, a.dtype) for a in results] + [pltpu.SemaphoreType.DMA((2, 3, 4))],
        compiler_params=pltpu.CompilerParams(vmem_limit_bytes=VMEM_LIMIT),
        name="hand_over",
    )(both, qkv)


def solution(mesh):
    n_devs = mesh.shape['ep']

    def local_step(x_a, route_a, gate_a, h_b, attn_b, route_b, gate_b, w_qkv, w_o, w_gate, w_up, w_down):
        tok_n, dim = x_a.shape
        top_k = route_a.shape[1]
        local_n, _, ff = w_gate.shape
        n_experts = local_n * n_devs
        capacity = min(tok_n, 2 * ((tok_n * top_k + n_experts - 1) // n_experts))
        row_n, n_slots, cols = n_devs * capacity, local_n * capacity, dim // CHUNKS
        half, n_chips = cols // 2, n_devs // 2

        any_spec = pl.BlockSpec(memory_space=pl.ANY)
        dma = pltpu.SemaphoreType.DMA

        def body(*refs):
            moe_kernel(capacity, *refs)

        flops = 2 * (6 * local_n * row_n * dim * ff + 8 * n_devs * n_slots * tok_n * dim) + 2 * tok_n * dim * 4 * dim
        both, qkv_b, _ = pl.pallas_call(
            body,
            in_specs=[any_spec] * 3 + [pl.BlockSpec(memory_space=pltpu.VMEM)] * 4 + [any_spec] * 5,
            out_specs=[any_spec] * 3,
            out_shape=[
                jax.ShapeDtypeStruct((2, tok_n, dim), BF16),
                jax.ShapeDtypeStruct((tok_n, w_qkv.shape[1]), BF16),
                jax.ShapeDtypeStruct((2, n_devs, tok_n, dim), BF16),
            ],
            scratch_shapes=[
                pltpu.VMEM((SLOTS, 2, dim, max(cols, 2 * WIDE)), BF16),
                pltpu.VMEM((local_n, row_n, dim), BF16),
                pltpu.VMEM((local_n, row_n, ff), BF16),
                pltpu.VMEM((n_devs, 2, 2 * local_n, tok_n), F32),
                pltpu.VMEM((2, tok_n, dim), BF16),
                pltpu.VMEM((n_devs, 3 * tok_n, n_slots), BF16),
                pltpu.VMEM((3, n_chips, 2, tok_n, half), F32),
                pltpu.VMEM((CHUNKS, n_chips, 2, tok_n, half), F32),
                pltpu.VMEM((CHUNKS, 2, tok_n, half), F32),
                pltpu.VMEM((CHUNKS, 2, 2, tok_n, half), F32),
                pltpu.VMEM((CHUNKS, tok_n, cols), BF16),
                pltpu.VMEM((CHUNKS, tok_n, cols), BF16),
                pltpu.VMEM((n_devs, 2, 2 * local_n, tok_n), F32),
                dma((SLOTS, 2, 2)),
                dma((2, 11)),
                dma((2, 11)),
                dma((n_devs,)),
                dma((n_devs,)),
                dma((2,)),
                dma((CHUNKS,)),
                dma((CHUNKS,)),
                dma((CHUNKS,)),
                dma((CHUNKS,)),
                dma((CHUNKS, 2)),
                dma((CHUNKS, 2)),
                dma((CHUNKS, 2, 2)),
                dma((CHUNKS, 2, 2)),
                pltpu.SemaphoreType.REGULAR,
                pltpu.SemaphoreType.REGULAR,
            ],
            compiler_params=pltpu.CompilerParams(
                collective_id=0, has_side_effects=True, vmem_limit_bytes=VMEM_LIMIT
            ),
            cost_estimate=pl.CostEstimate(flops=flops, bytes_accessed=400_000_000, transcendentals=0),
            name="moe_step",
        )(x_a, h_b, attn_b, route_a.T, gate_a.T, route_b.T, gate_b.T, w_qkv, w_o, w_gate, w_up, w_down)
        return tuple(hand_over(both, qkv_b))

    row_spec = P(('dp', 'ep'), None)
    full_spec = P(None, None)
    expert_spec = P('ep', None, None)
    return jax.shard_map(
        local_step,
        mesh=mesh,
        in_specs=(row_spec, row_spec, row_spec, row_spec, row_spec, row_spec, row_spec, full_spec, full_spec, expert_spec, expert_spec, expert_spec),
        out_specs=(row_spec, row_spec, row_spec),
        check_vma=False,
    )
```
